32 devices in a mesh: spin: 2 (over core), band: 8 (over z, x), grid: 2 (over y).
Axes of the slice: x: 2, y: 2, z: 4, core: 2. Of those that a mesh axis runs over, the one named last changes fastest.
Arguments:
- orbitals: bfloat16 [2, 64, 128, 128, 128], P('spin', 'band', 'grid'), may hold values from -0.14941406 to 0.14941406
- partial_bands: int32 [2, 2], P('spin'), may hold values from 0 to 63
- core_density: float32 [128, 128, 128], P('grid'), may hold values from 0.002 to 0.2
Outputs:
- potential: float32 [2, 128, 128, 128], P('spin', 'grid', 'band')
The draws below stay inside these ranges and needn't reach their ends.
Inputs may be any that keep to these rules, and one draw needn't show every extreme that they name: `partial_bands`: row s holds, for spin s, the first half-occupied band and the count of half-occupied bands; bands past 64 - 1 do not exist.
All inputs are finite; a program needn't handle non-finite values.
Results may differ from the reference program's by a relative error of at most 0.0003.
Values sent between devices are 32-bit elements; how exact they have to be, the bound alone decides.
A program may use at most 128 MiB of HBM per device.

```python
import math
import jax
import jax.numpy as jnp
from jax import lax

NX = 128
NY = 128
NZ = 128
SPINS = 2
BANDS = 64


def set_ends(drawn, own_key, smallest, high):
    extent = drawn.shape
    spot = [jax.random.randint(jax.random.fold_in(own_key, axis), (), 0, extent[axis]) for axis in range(len(extent))]
    drawn = drawn.at[tuple(spot)].set(smallest)
    longest = extent.index(max(extent))
    spot[longest] = (spot[longest] + 1) % extent[longest]
    return drawn.at[tuple(spot)].set(high)


def shard_levels(own_key, shape, pieces, least, top_value):
    def one(axis_at, parts):
        steps = jax.random.uniform(jax.random.fold_in(jax.random.fold_in(own_key, 6), axis_at), (parts,), jnp.float32, least / len(pieces), top_value / len(pieces))
        return jnp.repeat(jnp.exp(steps), shape[axis_at] // parts).reshape((-1,) + (1,) * (len(shape) - axis_at - 1))

    factor_of = one(*pieces[0])
    for cut in pieces[1:]:
        factor_of = factor_of * one(*cut)
    return factor_of


def noise(key, shape, scale, reach, cuts=(), kind=jnp.bfloat16):
    drawn = scale * jax.random.normal(key, shape, jnp.float32)
    if cuts:
        drawn = drawn * shard_levels(key, shape, cuts, -0.22, 0.18)
    return jnp.clip(drawn, -reach, reach).astype(kind)


def setup_inputs(seed: int = 0) -> dict:
    arg_keys = jax.random.split(jax.random.key(seed), 4)
    return {
        "orbitals": noise(arg_keys[0], (SPINS, BANDS, NX, NY, NZ), 0.025, 0.14941406, ((0, 2), (1, 8), (2, 2))),
        "partial_bands": set_ends(jax.random.randint(arg_keys[1], (SPINS, 2), 0, BANDS), jax.random.fold_in(arg_keys[1], 1), 0, BANDS - 1).astype(jnp.int32),
        "core_density": jnp.clip(jnp.exp(math.log(0.2) - 4.6051702 * jax.random.uniform(arg_keys[2], (NX, NY, NZ), jnp.float32) ** shard_levels(arg_keys[2], (NX, NY, NZ), ((0, 2),), -0.2, 0.2)), 0.002, 0.2),
    }


KAPPA = 0.804
MU_X = 0.2195149727645171
BETA = 0.06672455060314922
GAMMA = (1.0 - math.log(2.0)) / math.pi ** 2
FZ_NORM = 2.0 ** (4.0 / 3.0) - 2.0
FPP_ZERO = 1.709921

def pw_fit(radius, amp, alpha, beta_one, beta_two, beta_three, beta_four):
    root = jnp.sqrt(radius)
    denom = 2.0 * amp * (beta_one * root + beta_two * radius + beta_three * radius * root + beta_four * radius * radius)
    return -2.0 * amp * (1.0 + alpha * radius) * jnp.log(1.0 + 1.0 / denom)

def exchange_part(double, sigma_four):
    kfermi = (3.0 * math.pi ** 2 * double) ** (1.0 / 3.0)
    scaled = sigma_four / (4.0 * kfermi * kfermi * double * double)
    enhance = 1.0 + KAPPA - KAPPA / (1.0 + MU_X * scaled / KAPPA)
    return -0.75 / math.pi * kfermi * double * enhance

def xc_energy(n_up, n_down, s_uu, s_ud, s_dd):
    exch = 0.5 * (exchange_part(2.0 * n_up, 4.0 * s_uu) + exchange_part(2.0 * n_down, 4.0 * s_dd))
    total = n_up + n_down
    zeta = (n_up - n_down) / total
    radius = (3.0 / (4.0 * math.pi * total)) ** (1.0 / 3.0)
    ec_para = pw_fit(radius, 0.031091, 0.2137, 7.5957, 3.5876, 1.6382, 0.49294)
    ec_ferro = pw_fit(radius, 0.015545, 0.20548, 14.1189, 6.1977, 3.3662, 0.62517)
    neg_stiff = pw_fit(radius, 0.016887, 0.11125, 10.357, 3.6231, 0.88026, 0.49671)
    plus_z = 1.0 + zeta
    minus_z = 1.0 - zeta
    fzeta = (plus_z ** (4.0 / 3.0) + minus_z ** (4.0 / 3.0) - 2.0) / FZ_NORM
    zeta_four = zeta ** 4
    ec_lda = ec_para - neg_stiff * fzeta / FPP_ZERO * (1.0 - zeta_four) + (ec_ferro - ec_para) * fzeta * zeta_four
    phi = 0.5 * (plus_z ** (2.0 / 3.0) + minus_z ** (2.0 / 3.0))
    phi_cube = phi * phi * phi
    kfermi = (3.0 * math.pi ** 2 * total) ** (1.0 / 3.0)
    screen_sq = 4.0 * kfermi / math.pi
    sigma = s_uu + 2.0 * s_ud + s_dd
    tsq = sigma / (4.0 * phi * phi * screen_sq * total * total)
    amp = BETA / GAMMA / (jnp.exp(-ec_lda / (GAMMA * phi_cube)) - 1.0)
    atsq = amp * tsq
    gradient_term = GAMMA * phi_cube * jnp.log(1.0 + BETA / GAMMA * tsq * (1.0 + atsq) / (1.0 + atsq + atsq * atsq))
    return exch + total * (ec_lda + gradient_term)

def spectral(field, axis):
    length = field.shape[axis]
    index = jnp.arange(length, dtype=jnp.int32)
    mode = jnp.where(index < length // 2, index, index - length)
    mode = jnp.where(index == length // 2, 0, mode)
    wave = 2.0 * math.pi / length * mode.astype(jnp.float32)
    shape = [1, 1, 1]
    shape[axis] = length
    spec = jnp.fft.fft(field, axis=axis)
    return jnp.real(jnp.fft.ifft(spec * (1j * wave.reshape(shape)), axis=axis)).astype(jnp.float32)

def reference(orbitals, partial_bands, core_density):
    band_ids = jnp.arange(BANDS, dtype=jnp.int32)

    def spin_density(spin_id):
        first = partial_bands[spin_id, 0]
        span = partial_bands[spin_id, 1]
        weights = jnp.where((band_ids >= first) & (band_ids < first + span), 0.5, 1.0).astype(jnp.float32)

        def accumulate(total, item):
            weight, orbital = item
            values = orbital.astype(jnp.float32)
            return (total + weight * values * values, None)
        start = jnp.zeros((NX, NY, NZ), jnp.float32)
        total, unused = lax.scan(accumulate, start, (weights, orbitals[spin_id]))
        return total + 0.5 * core_density
    dens_up = spin_density(0)
    dens_down = spin_density(1)
    grad_up = [spectral(dens_up, axis) for axis in range(3)]
    grad_down = [spectral(dens_down, axis) for axis in range(3)]
    s_uu = grad_up[0] * grad_up[0] + grad_up[1] * grad_up[1] + grad_up[2] * grad_up[2]
    s_ud = grad_up[0] * grad_down[0] + grad_up[1] * grad_down[1] + grad_up[2] * grad_down[2]
    s_dd = grad_down[0] * grad_down[0] + grad_down[1] * grad_down[1] + grad_down[2] * grad_down[2]
    energy, pull = jax.vjp(xc_energy, dens_up, dens_down, s_uu, s_ud, s_dd)
    derivs = pull(jnp.ones_like(energy))
    div_up = jnp.zeros_like(dens_up)
    div_down = jnp.zeros_like(dens_up)
    for axis in range(3):
        flux_up = 2.0 * derivs[2] * grad_up[axis] + derivs[3] * grad_down[axis]
        flux_down = 2.0 * derivs[4] * grad_down[axis] + derivs[3] * grad_up[axis]
        div_up = div_up + spectral(flux_up, axis)
        div_down = div_down + spectral(flux_down, axis)
    return jnp.stack([derivs[0] - div_up, derivs[1] - div_down])
```

```python
import functools
import math

import jax
import jax.numpy as jnp
import numpy as np
from jax import lax
from jax.experimental import pallas as pl
from jax.experimental.pallas import tpu as pltpu
from jax.sharding import PartitionSpec as P

KAPPA = 0.804
MU_X = 0.2195149727645171
BETA = 0.06672455060314922
GAMMA = (1.0 - math.log(2.0)) / math.pi**2
FZ_NORM = 2.0 ** (4.0 / 3.0) - 2.0
FPP_ZERO = 1.709921
MESH = pl.DeviceIdType.MESH
CHUNK = 4
AHEAD = 3
LATE = 2
FAST = 2
XC_ROWS = 2
TILE = 8


def cube_root(value):
    return jnp.exp(jnp.log(value) * (1.0 / 3.0))


def pw_fit(radius, root, amp, alpha, beta_one, beta_two, beta_three, beta_four):
    denom = (2.0 * amp) * (
        root * (beta_one + root * (beta_two + root * (beta_three + root * beta_four)))
    )
    return -2.0 * amp * (1.0 + alpha * radius) * jnp.log(1.0 + 1.0 / denom)


def exchange_part(double, sigma_four):
    kfermi = (3.0 * math.pi**2) ** (1.0 / 3.0) * cube_root(double)
    product = kfermi * double
    scaled = sigma_four / (4.0 * product * product)
    enhance = 1.0 + KAPPA - KAPPA / (1.0 + MU_X * scaled / KAPPA)
    return -0.75 / math.pi * product * enhance


def xc_energy(n_up, n_down, s_uu, s_ud, s_dd):
    exch = 0.5 * (exchange_part(2.0 * n_up, 4.0 * s_uu) + exchange_part(2.0 * n_down, 4.0 * s_dd))
    total = n_up + n_down
    zeta = (n_up - n_down) / total
    third = cube_root(total)
    radius = (3.0 / (4.0 * math.pi)) ** (1.0 / 3.0) / third
    root = jnp.sqrt(radius)
    ec_para = pw_fit(radius, root, 0.031091, 0.2137, 7.5957, 3.5876, 1.6382, 0.49294)
    ec_ferro = pw_fit(radius, root, 0.015545, 0.20548, 14.1189, 6.1977, 3.3662, 0.62517)
    neg_stiff = pw_fit(radius, root, 0.016887, 0.11125, 10.357, 3.6231, 0.88026, 0.49671)
    plus_z = 1.0 + zeta
    minus_z = 1.0 - zeta
    plus_third = cube_root(plus_z)
    minus_third = cube_root(minus_z)
    fzeta = (plus_z * plus_third + minus_z * minus_third - 2.0) * (1.0 / FZ_NORM)
    zeta_sq = zeta * zeta
    zeta_four = zeta_sq * zeta_sq
    ec_lda = (
        ec_para
        - neg_stiff * fzeta * (1.0 / FPP_ZERO) * (1.0 - zeta_four)
        + (ec_ferro - ec_para) * fzeta * zeta_four
    )
    phi = 0.5 * (plus_third * plus_third + minus_third * minus_third)
    phi_cube = phi * phi * phi
    kfermi = (3.0 * math.pi**2) ** (1.0 / 3.0) * third
    screen_sq = kfermi * (4.0 / math.pi)
    sigma = s_uu + 2.0 * s_ud + s_dd
    tsq = sigma / (4.0 * phi * phi * screen_sq * total * total)
    amp = BETA / GAMMA / (jnp.exp(-ec_lda / (GAMMA * phi_cube)) - 1.0)
    atsq = amp * tsq
    gradient_term = (
        GAMMA
        * phi_cube
        * jnp.log(1.0 + BETA / GAMMA * tsq * (1.0 + atsq) / (1.0 + atsq + atsq * atsq))
    )
    return exch + total * (ec_lda + gradient_term)


def spectral_table(length):
    index = np.arange(length)
    angle = 2.0 * np.pi / length * (index[:, None] * index[None, :] % length)
    mode = np.where(index < length // 2, index, index - length)
    mode = np.where(index == length // 2, 0, mode)
    wave = 2.0 * np.pi / length * mode
    sines, cosines = np.sin(angle), np.cos(angle)
    first_term = (sines * wave[None, :]) @ cosines.T
    second_term = (cosines * wave[None, :]) @ sines.T
    return (second_term - first_term) / length


def halves_of_table(table):
    high = table.astype(jnp.bfloat16)
    low = (table - high.astype(np.float64)).astype(jnp.bfloat16)
    return high, low


def left_table(table):
    high, low = halves_of_table(table)
    return np.concatenate([np.concatenate([part, part], axis=1) for part in (high, low)], axis=0)


def right_table(table):
    high, low = halves_of_table(table)
    both = np.concatenate([high, low], axis=1)
    return np.concatenate([both, both], axis=0)


def halves(field):
    high = field.astype(jnp.bfloat16)
    return high, (field - high.astype(jnp.float32)).astype(jnp.bfloat16)


def from_left(table, field):
    product = jnp.dot(
        table, jnp.concatenate(halves(field), axis=0), preferred_element_type=jnp.float32
    )
    rows = product.shape[0] // 2
    return product[:rows] + product[rows:]


def from_right(field, table):
    product = jnp.dot(
        jnp.concatenate(halves(field), axis=1), table, preferred_element_type=jnp.float32
    )
    columns = product.shape[1] // 2
    return product[:, :columns] + product[:, columns:]


def potential_kernel(
    bands,
    grids,
    pairs_ref,
    orb_hbm,
    core_hbm,
    tx_ref,
    ty_ref,
    tz_ref,
    out_ref,
    orb,
    core,
    part,
    x_in,
    z_out,
    z_in,
    own,
    gx,
    hx,
    nx,
    gy,
    hy,
    ny,
    dz,
    n_twin,
    nx_twin,
    fx,
    fx_out,
    fy,
    fz,
    s_out,
    base,
    sy,
    orb_sem,
    core_sem,
    x_send,
    x_recv,
    z_send,
    z_recv,
    g_send,
    g_recv,
    n_send,
    n_recv,
    nx_send,
    nx_recv,
    yf_send,
    yf_recv,
    yb_send,
    yb_twin,
    yb_recv,
    fy_send,
    fy_other,
    fy_recv,
    fx_send,
    fx_recv,
    s_send,
    s_recv,
    sb_send,
    sb_recv,
):
    count, rows, y_cells, z_cells = orb.shape
    block = core.shape[1]
    slow = bands // FAST
    chunk = x_in.shape[1] // x_recv.shape[0]
    chunks = rows // chunk
    per_unit = TILE // chunk
    units = rows // (2 * TILE)
    groups = rows // bands
    per_group = bands // chunk
    pair_groups = 2 * TILE // bands
    me = lax.axis_index("band")
    slab = lax.axis_index("grid")
    spin = lax.axis_index("spin")
    place, fast = lax.div(me, FAST), lax.rem(me, FAST)
    across = {"band": place * FAST + (1 - fast)}
    twin = {"spin": 1 - spin}
    my_block = pl.ds(pl.multiple_of(me * block, TILE), block)

    def remote(src, dst, send, recv, device):
        return pltpu.make_async_remote_copy(
            src_ref=src,
            dst_ref=dst,
            send_sem=send,
            recv_sem=recv,
            device_id=device,
            device_id_type=MESH,
        )

    def take(ref, sem):
        pltpu.make_async_copy(ref, ref, sem).wait()

    def each(number, body):
        lax.fori_loop(0, number, lambda i, carry: (body(i), carry)[1], 0)

    def chunk_span(c):
        return pl.ds(c * chunk, chunk)

    def unit_rows(w):
        return pl.ds(pl.multiple_of(w * TILE, TILE), TILE)

    def line_rows(w):
        return pl.ds(pl.multiple_of(slab * rows + w * TILE, TILE), TILE)

    def band_block(j):
        return pl.ds(pl.multiple_of(j * block, TILE), block)

    def turned(value):
        return jnp.transpose(value, (1, 0, 2))

    def orb_copy(c):
        span = chunk_span(c)
        return pltpu.make_async_copy(orb_hbm.at[0, :, span], orb.at[:, span], orb_sem.at[c])

    def core_copy():
        return pltpu.make_async_copy(core_hbm.at[:, my_block], core, core_sem)

    def x_copy(c):
        span = chunk_span(c)
        return remote(part.at[1 - fast, :, span], x_in.at[:, span], x_send, x_recv.at[c], across)

    def z_copy(c, d, slot, to):
        span = chunk_span(c)
        return remote(
            z_out.at[d, span],
            z_in.at[slot, span],
            z_send,
            z_recv.at[c, slot],
            {"band": to * FAST + fast},
        )

    def gather_copy(w, k):
        return remote(
            gx.at[0, :, line_rows(w)],
            gx.at[0, :, line_rows(w)],
            g_send.at[w, k - 1],
            g_recv.at[w, k - 1],
            {"grid": lax.rem(slab + k, grids)},
        )

    def n_copy(v):
        return remote(
            own.at[unit_rows(2 * v + 1 - spin)], n_twin.at[v], n_send.at[v], n_recv.at[v], twin
        )

    def nx_copy(v):
        return remote(
            nx.at[unit_rows(2 * v + 1 - spin)], nx_twin.at[v], nx_send.at[v], nx_recv.at[v], twin
        )

    def fx_same(v, k):
        return remote(
            gx.at[1, :, line_rows(2 * v + spin)],
            gx.at[1, :, line_rows(2 * v + spin)],
            fx_send.at[0, v, k],
            fx_recv.at[0, v, k],
            {"grid": lax.rem(slab + k, grids)},
        )

    def fx_cross(v, k):
        return remote(
            fx_out.at[v],
            gx.at[1, :, line_rows(2 * v + spin)],
            fx_send.at[1, v, k],
            fx_recv.at[1, v, k],
            {"spin": 1 - spin, "grid": lax.rem(slab + k, grids)},
        )

    def s_copy(v):
        return remote(
            s_out.at[v], base.at[unit_rows(2 * v + spin)], s_send.at[v], s_recv.at[v], twin
        )

    def my_row(i):
        row = i * bands + me
        unit = lax.div(row, TILE)
        return row, lax.rem(unit, 2), lax.div(unit, 2), lax.rem(row, TILE)

    def yb_copy(i, j, send):
        row, holder, v, e = my_row(i)
        slot = jnp.where(holder == spin, 0, 1)
        return remote(
            hy.at[0, i, band_block(j)],
            ny.at[slot, v, e],
            send,
            yb_recv.at[slot, v, e],
            {"spin": holder, "band": j},
        )

    def fy_own(v, e, i, q):
        return remote(
            fy.at[0, v, e],
            gy.at[1, i, my_block],
            fy_send.at[v, e],
            fy_recv.at[i, 0],
            {"band": q},
        )

    def fy_cross(v, e, i, q):
        return remote(
            fy.at[1, v, e],
            gy.at[1, i, my_block],
            fy_other,
            fy_recv.at[i, jnp.where(q == me, 1, 0)],
            {"spin": 1 - spin, "band": q},
        )

    def sb_copy(i, k):
        q = lax.rem(me + k, bands)
        return remote(
            hy.at[1, i, band_block(q)],
            sy.at[i * bands + me],
            sb_send,
            sb_recv.at[i],
            {"band": q},
        )

    each(chunks, lambda c: orb_copy(c).start())
    core_copy().start()
    barrier = pltpu.get_barrier_semaphore()
    partners = [{"spin": 1 - spin}]
    for core_id in (spin, 1 - spin):
        partners += [{"spin": core_id, "band": lax.rem(me + k, bands)} for k in range(1, bands)]
        partners += [{"spin": core_id, "grid": lax.rem(slab + k, grids)} for k in range(1, grids)]
    for target in partners:
        pl.semaphore_signal(barrier, inc=1, device_id=target, device_id_type=MESH)
    first = pairs_ref[0, 0]
    last = first + pairs_ref[0, 1]
    weights = []
    for n in range(count):
        ident = me * count + n
        weights.append(jnp.where((ident >= first) & (ident < last), 0.5, 1.0).astype(jnp.float32))

    def squares(c):
        orb_copy(c).wait()
        for r in range(chunk):
            row = c * chunk + r
            for b in range(bands):
                total = jnp.zeros((block, z_cells), jnp.float32)
                for n in range(count):
                    values = orb[n, row, b * block : (b + 1) * block].astype(jnp.float32)
                    total += weights[n] * (values * values)
                part[b % FAST, b // FAST, row] = total

    def sum_across(c):
        x_copy(c).wait_recv()
        span = chunk_span(c)
        for d in range(slow):
            z_out[d, span] = part[fast, d, span] + x_in[d, span]

        @pl.when(place == 0)
        def _():
            for d in range(slow - 1, 0, -1):
                z_copy(c, d, d, 1).start()

        @pl.when(place == slow - 1)
        def _():
            for d in range(slow - 1):
                z_copy(c, d, slow if d == slow - 2 else d, slow - 2).start()

    def hop(h, c):
        span = chunk_span(c)

        @pl.when(place == h)
        def _():
            for d in range(slow - 1, h - 1, -1):
                z_copy(c, d, d, h).wait_recv()
                z_out[d, span] += z_in[d, span]
                if d > h:
                    z_copy(c, d, d, h + 1).start()

        at = slow - 1 - h

        @pl.when(place == at)
        def _():
            for d in range(at + 1):
                slot = slow if d == at else d
                z_copy(c, d, slot, at).wait_recv()
                z_out[d, span] += z_in[slot, span]
                if d < at:
                    z_copy(c, d, slow if d == at - 1 else d, at - 1).start()

    def collect(c):
        span = chunk_span(c)
        own[span] = 0.5 * core[span] + z_out[place, span]
        for r in range(chunk):
            row = c * chunk + r
            i, q = lax.div(row, bands), lax.rem(row, bands)

            @pl.when(q != me)
            def _():
                remote(
                    own.at[row], gy.at[0, i, my_block], yf_send, yf_recv.at[i], {"band": q}
                ).start()

            @pl.when(q == me)
            def _():
                gy[0, i, my_block] = own[row]

    def share(w):
        v = lax.div(w, 2)
        gx[0, :, line_rows(w)] = turned(own[unit_rows(w)])
        for k in range(1, grids):
            gather_copy(w, k).start()

        @pl.when(lax.rem(w, 2) != spin)
        def _():
            n_copy(v).start()

        @pl.when(lax.rem(w, 2) == spin)
        def _():
            field = own[unit_rows(w)].reshape(TILE * block, z_cells)
            dz[0, v] = from_right(field, tz_ref[...]).reshape(TILE, block, z_cells)

    def steep_second(i):
        take(gy.at[0, i, pl.ds(0, (bands - 1) * block)], yf_recv.at[i])
        hy[0, i] = from_left(ty_ref[...], gy[0, i])
        for k in range(1, bands):
            yb_copy(i, lax.rem(me + k, bands), yb_send).start()
        row, holder, v, e = my_row(i)

        @pl.when(holder == spin)
        def _():
            ny[0, v, e] = hy[0, i, my_block]

        @pl.when(holder != spin)
        def _():
            yb_copy(i, me, yb_twin.at[i]).start()

    def along_first(t):
        table = tx_ref[slab]
        for y in range(0, block, 2):
            pair = jnp.concatenate([gx[t, y], gx[t, y + 1]], axis=1)
            product = from_left(table, pair)
            hx[y] = product[:, :z_cells]
            hx[y + 1] = product[:, z_cells:]

    ahead = min(AHEAD, chunks)
    for c in range(ahead):
        squares(c)
        if c == 0:
            pl.semaphore_wait(barrier, len(partners))
        x_copy(c).start()
    core_copy().wait()
    end = chunks + slow - 1 + LATE

    def step(u):
        @pl.when(u + ahead < chunks)
        def _():
            squares(u + ahead)
            x_copy(u + ahead).start()

        @pl.when(u < chunks)
        def _():
            sum_across(u)

        for h in range(1, slow):

            @pl.when((u >= h) & (u < chunks + h))
            def _():
                hop(h, u - h)

        done = u - (slow - 1)

        @pl.when((done >= 0) & (done < chunks))
        def _():
            collect(done)

            @pl.when(lax.rem(done, per_unit) == per_unit - 1)
            def _():
                share(lax.div(done, per_unit))

        late = done - LATE

        @pl.when((late >= 0) & (lax.rem(late, per_group) == per_group - 1))
        def _():
            @pl.when(late < chunks - per_group)
            def _():
                steep_second(lax.div(late, per_group))

    each(end - LATE, step)

    for v in range(units):
        n_copy(v).wait_recv()
        field = n_twin[v].reshape(TILE * block, z_cells)
        dz[1, v] = from_right(field, tz_ref[...]).reshape(TILE, block, z_cells)
    for w in range(2 * units):
        for k in range(1, grids):
            gather_copy(w, k).wait_recv()
    along_first(0)
    nx[...] = turned(hx[...])
    for v in range(units):
        nx_copy(v).start()
    steps_done = [
        g for g in range(groups) if (g + 1) * per_group - 1 + LATE + slow - 1 < end - LATE
    ]
    done_groups = len([g for g in steps_done if (g + 1) * per_group - 1 < chunks - per_group])
    for g in range(done_groups, groups):
        steep_second(g)

    def potential_rows(v, e):
        span = pl.ds(e, XC_ROWS)
        here = pl.ds((2 * v + spin) * TILE + e, XC_ROWS)
        n_own, n_other = own[here], n_twin[v, span]
        g_own = [nx[here], ny[0, v, span], dz[0, v, span]]
        g_other = [nx_twin[v, span], ny[1, v, span], dz[1, v, span]]
        s_own = g_own[0] * g_own[0] + g_own[1] * g_own[1] + g_own[2] * g_own[2]
        s_mix = g_own[0] * g_other[0] + g_own[1] * g_other[1] + g_own[2] * g_other[2]
        s_other = g_other[0] * g_other[0] + g_other[1] * g_other[1] + g_other[2] * g_other[2]
        energy, pull = jax.vjp(xc_energy, n_own, n_other, s_own, s_mix, s_other)
        derivs = pull(jnp.ones_like(energy))
        base[here] = derivs[0]
        s_out[v, span] = derivs[1]
        flux = [
            [2.0 * derivs[2] * g_own[a] + derivs[3] * g_other[a] for a in range(3)],
            [2.0 * derivs[4] * g_other[a] + derivs[3] * g_own[a] for a in range(3)],
        ]
        for slot in range(2):
            fx[slot, span] = flux[slot][0]
            fy[slot, v, span] = flux[slot][1]
            fz[slot, span] = flux[slot][2]
        for r in range(XC_ROWS):
            row = (2 * v + spin) * TILE + e + r
            i, q = lax.div(row, bands), lax.rem(row, bands)
            fy_cross(v, e + r, i, q).start()

            @pl.when(q != me)
            def _():
                fy_own(v, e + r, i, q).start()

            @pl.when(q == me)
            def _():
                gy[1, i, my_block] = fy[0, v, e + r]

    def evaluate(v):
        for e in range(TILE):
            row = (2 * v + spin) * TILE + e

            @pl.when(lax.rem(row, bands) != me)
            def _():
                take(ny.at[0, v, e], yb_recv.at[0, v, e])

            take(ny.at[1, v, e], yb_recv.at[1, v, e])
        nx_copy(v).wait_recv()
        each(TILE // XC_ROWS, lambda e: potential_rows(v, e * XC_ROWS))
        gx[1, :, line_rows(2 * v + spin)] = turned(fx[0])
        fx_out[v] = turned(fx[1])
        for k in range(grids):
            if k > 0:
                fx_same(v, k).start()
            fx_cross(v, k).start()
        for slot in range(2):
            field = fz[slot].reshape(TILE * block, z_cells)
            slope = from_right(field, tz_ref[...]).reshape(TILE, block, z_cells)
            if slot == 0:
                mine = unit_rows(2 * v + spin)
                base[mine] = base[mine] - slope
            else:
                s_out[v] = s_out[v] - slope
        s_copy(v).start()

    def flux_second(i):
        take(gy.at[1, i, pl.ds(0, (bands - 1) * block)], fy_recv.at[i, 0])
        row, holder, v, e = my_row(i)

        @pl.when(holder != spin)
        def _():
            take(gy.at[1, i, pl.ds(0, block)], fy_recv.at[i, 1])

        hy[1, i] = from_left(ty_ref[...], gy[1, i])
        for k in range(1, bands):
            sb_copy(i, k).start()
        sy[row] = hy[1, i, my_block]

    def unit_step(v):
        evaluate(v)

        @pl.when(v >= 1)
        def _():
            each(pair_groups, lambda g: flux_second((v - 1) * pair_groups + g))

    each(units, unit_step)
    each(pair_groups, lambda g: flux_second((units - 1) * pair_groups + g))

    for v in range(units):
        for k in range(grids):
            if k > 0:
                fx_same(v, k).wait_recv()
            fx_cross(v, k).wait_recv()
    along_first(1)
    for v in range(units):
        s_copy(v).wait_recv()
    base[...] = base[...] - turned(hx[...])

    take(part.at[0], x_send)
    take(z_out.at[pl.ds(0, slow - 1)], z_send)
    take(own.at[pl.ds(0, rows - groups)], yf_send)
    take(sy.at[pl.ds(0, groups * (bands - 1))], yb_send)
    for g in range(groups):
        row, holder, v, e = my_row(g)

        @pl.when(holder != spin)
        def _():
            take(sy.at[0], yb_twin.at[g])

    take(fy.at[1], fy_other)

    def drain(v):
        n_copy(v).wait_send()
        nx_copy(v).wait_send()
        s_copy(v).wait_send()
        for k in range(grids):
            if k > 0:
                fx_same(v, k).wait_send()
                gather_copy(2 * v, k).wait_send()
                gather_copy(2 * v + 1, k).wait_send()
            fx_cross(v, k).wait_send()
        for e in range(TILE):
            row = (2 * v + spin) * TILE + e

            @pl.when(lax.rem(row, bands) != me)
            def _():
                take(fy.at[0, v, e], fy_send.at[v, e])

    each(units, drain)

    def finish(i):
        take(sy.at[pl.ds(0, bands - 1)], sb_recv.at[i])
        span = pl.ds(i * bands, bands)
        out_ref[span] = base[span] - sy[span]

    each(groups, finish)
    take(sy.at[pl.ds(0, groups * (bands - 1))], sb_send)


def potential_call(orbitals, partial_bands, core_density, tables):
    bands, grids = lax.axis_size("band"), lax.axis_size("grid")
    _, count, rows, y_cells, z_cells = orbitals.shape
    block, slow = y_cells // bands, bands // FAST
    x_cells = rows * grids
    chunk = min(CHUNK, TILE)
    chunks = rows // chunk
    units, groups = rows // (2 * TILE), rows // bands
    vmem = pl.BlockSpec(memory_space=pltpu.VMEM)
    hbm = pl.BlockSpec(memory_space=pl.ANY)
    dma = pltpu.SemaphoreType.DMA
    real = jnp.float32

    def held(*shape):
        return pltpu.VMEM(shape + (z_cells,), real)

    return pl.pallas_call(
        functools.partial(potential_kernel, bands, grids),
        out_shape=jax.ShapeDtypeStruct((rows, block, z_cells), real),
        in_specs=[pl.BlockSpec(memory_space=pltpu.SMEM), hbm, hbm] + [vmem] * 3,
        out_specs=vmem,
        scratch_shapes=[
            pltpu.VMEM((count, rows, y_cells, z_cells), jnp.bfloat16),
            held(rows, block),
            held(FAST, slow, rows, block),
            held(slow, rows, block),
            held(slow, rows, block),
            held(slow + 1, rows, block),
            held(rows, block),
            held(2, block, x_cells),
            held(block, rows),
            held(rows, block),
            held(2, groups, y_cells),
            held(2, groups, y_cells),
            held(2, units, TILE, block),
            held(2, units, TILE, block),
            held(units, TILE, block),
            held(units, TILE, block),
            held(2, TILE, block),
            held(units, block, TILE),
            held(2, units, TILE, block),
            held(2, TILE, block),
            held(units, TILE, block),
            held(rows, block),
            held(rows, block),
            dma((chunks,)),
            dma,
            dma,
            dma((chunks,)),
            dma,
            dma((chunks, slow + 1)),
            dma((2 * units, grids - 1)),
            dma((2 * units, grids - 1)),
            dma((units,)),
            dma((units,)),
            dma((units,)),
            dma((units,)),
            dma,
            dma((groups,)),
            dma,
            dma((groups,)),
            dma((2, units, TILE)),
            dma((units, TILE)),
            dma,
            dma((groups, 2)),
            dma((2, units, grids)),
            dma((2, units, grids)),
            dma((units,)),
            dma((units,)),
            dma,
            dma((groups,)),
        ],
        compiler_params=pltpu.CompilerParams(
            collective_id=0, has_side_effects=True, vmem_limit_bytes=60 * 2**20
        ),
        name="potential",
    )(partial_bands, orbitals, core_density, *tables)


def per_device(orbitals, partial_bands, core_density):
    rows, y_cells, z_cells = core_density.shape
    grids = lax.axis_size("grid")
    table = spectral_table(rows * grids)
    slabs = [left_table(table[g * rows : (g + 1) * rows]) for g in range(grids)]
    tables = (
        jnp.asarray(np.stack(slabs)),
        jnp.asarray(left_table(spectral_table(y_cells))),
        jnp.asarray(right_table(spectral_table(z_cells).T)),
    )
    return potential_call(orbitals, partial_bands, core_density, tables)[None]


def solution(mesh):
    in_specs = (P("spin", "band", "grid", None, None), P("spin", None), P("grid", None, None))
    out_specs = P("spin", "grid", "band", None)
    return jax.shard_map(
        per_device, mesh=mesh, in_specs=in_specs, out_specs=out_specs, check_vma=False
    )
```

```python
import functools
import math

import jax
import jax.numpy as jnp
import numpy as np
from jax import lax
from jax.experimental import pallas as pl
from jax.experimental.pallas import tpu as pltpu
from jax.sharding import PartitionSpec as P

KAPPA = 0.804
MU_X = 0.2195149727645171
BETA = 0.06672455060314922
GAMMA = (1.0 - math.log(2.0)) / math.pi**2
FZ_NORM = 2.0 ** (4.0 / 3.0) - 2.0
FPP_ZERO = 1.709921
MESH = pl.DeviceIdType.MESH
CHUNK = 4
AHEAD = 3
LATE = 2
AFTER = 1
BEHIND = 3
FIRSTS = 2
FIRST_STEP = 2
FIRST_LAG = 1
FIRST_LATE = 3
FAST = 2
XC_ROWS = 2
TILE = 8


def cube_root(value):
    return jnp.exp(jnp.log(value) * (1.0 / 3.0))


def pw_fit(radius, root, amp, alpha, beta_one, beta_two, beta_three, beta_four):
    denom = (2.0 * amp) * (
        root * (beta_one + root * (beta_two + root * (beta_three + root * beta_four)))
    )
    return -2.0 * amp * (1.0 + alpha * radius) * jnp.log(1.0 + 1.0 / denom)


def exchange_part(double, sigma_four):
    kfermi = (3.0 * math.pi**2) ** (1.0 / 3.0) * cube_root(double)
    product = kfermi * double
    scaled = sigma_four / (4.0 * product * product)
    enhance = 1.0 + KAPPA - KAPPA / (1.0 + MU_X * scaled / KAPPA)
    return -0.75 / math.pi * product * enhance


def xc_energy(n_up, n_down, s_uu, s_ud, s_dd):
    exch = 0.5 * (exchange_part(2.0 * n_up, 4.0 * s_uu) + exchange_part(2.0 * n_down, 4.0 * s_dd))
    total = n_up + n_down
    zeta = (n_up - n_down) / total
    third = cube_root(total)
    radius = (3.0 / (4.0 * math.pi)) ** (1.0 / 3.0) / third
    root = jnp.sqrt(radius)
    ec_para = pw_fit(radius, root, 0.031091, 0.2137, 7.5957, 3.5876, 1.6382, 0.49294)
    ec_ferro = pw_fit(radius, root, 0.015545, 0.20548, 14.1189, 6.1977, 3.3662, 0.62517)
    neg_stiff = pw_fit(radius, root, 0.016887, 0.11125, 10.357, 3.6231, 0.88026, 0.49671)
    plus_z = 1.0 + zeta
    minus_z = 1.0 - zeta
    plus_third = cube_root(plus_z)
    minus_third = cube_root(minus_z)
    fzeta = (plus_z * plus_third + minus_z * minus_third - 2.0) * (1.0 / FZ_NORM)
    zeta_sq = zeta * zeta
    zeta_four = zeta_sq * zeta_sq
    ec_lda = (
        ec_para
        - neg_stiff * fzeta * (1.0 / FPP_ZERO) * (1.0 - zeta_four)
        + (ec_ferro - ec_para) * fzeta * zeta_four
    )
    phi = 0.5 * (plus_third * plus_third + minus_third * minus_third)
    phi_cube = phi * phi * phi
    kfermi = (3.0 * math.pi**2) ** (1.0 / 3.0) * third
    screen_sq = kfermi * (4.0 / math.pi)
    sigma = s_uu + 2.0 * s_ud + s_dd
    tsq = sigma / (4.0 * phi * phi * screen_sq * total * total)
    amp = BETA / GAMMA / (jnp.exp(-ec_lda / (GAMMA * phi_cube)) - 1.0)
    atsq = amp * tsq
    gradient_term = (
        GAMMA
        * phi_cube
        * jnp.log(1.0 + BETA / GAMMA * tsq * (1.0 + atsq) / (1.0 + atsq + atsq * atsq))
    )
    return exch + total * (ec_lda + gradient_term)


def spectral_table(length):
    index = np.arange(length)
    angle = 2.0 * np.pi / length * (index[:, None] * index[None, :] % length)
    mode = np.where(index < length // 2, index, index - length)
    mode = np.where(index == length // 2, 0, mode)
    wave = 2.0 * np.pi / length * mode
    sines, cosines = np.sin(angle), np.cos(angle)
    first_term = (sines * wave[None, :]) @ cosines.T
    second_term = (cosines * wave[None, :]) @ sines.T
    return (second_term - first_term) / length


def halves_of_table(table):
    high = table.astype(jnp.bfloat16)
    low = (table - high.astype(np.float64)).astype(jnp.bfloat16)
    return high, low


def left_table(table):
    high, low = halves_of_table(table)
    return np.concatenate([np.concatenate([part, part], axis=1) for part in (high, low)], axis=0)


def right_table(table):
    high, low = halves_of_table(table)
    both = np.concatenate([high, low], axis=1)
    return np.concatenate([both, both], axis=0)


def halves(field):
    high = field.astype(jnp.bfloat16)
    return high, (field - high.astype(jnp.float32)).astype(jnp.bfloat16)


def from_left(table, field):
    product = jnp.dot(
        table, jnp.concatenate(halves(field), axis=0), preferred_element_type=jnp.float32
    )
    rows = product.shape[0] // 2
    return product[:rows] + product[rows:]


def from_right(field, table):
    product = jnp.dot(
        jnp.concatenate(halves(field), axis=1), table, preferred_element_type=jnp.float32
    )
    columns = product.shape[1] // 2
    return product[:, :columns] + product[:, columns:]


def potential_kernel(
    bands,
    grids,
    pairs_ref,
    orb_hbm,
    core_hbm,
    tx_hbm,
    ty_hbm,
    tz_hbm,
    out_ref,
    orb,
    core,
    part,
    x_in,
    z_out,
    z_in,
    f_in,
    fx_in,
    tx,
    ty,
    tz,
    own,
    gx,
    hx,
    nx,
    gy,
    hy,
    ny,
    dz,
    n_twin,
    nx_twin,
    fx,
    fx_out,
    fy,
    fz,
    s_out,
    base,
    sy,
    orb_sem,
    core_sem,
    x_send,
    x_recv,
    z_send,
    z_recv,
    f_send,
    f_recv,
    fe_send,
    fe_recv,
    table_sem,
    out_sem,
    line_sem,
    across_sem,
    g_send,
    g_recv,
    n_send,
    n_recv,
    nx_send,
    nx_recv,
    yf_send,
    yf_recv,
    yb_send,
    yb_twin,
    yb_recv,
    fy_send,
    fy_other,
    fy_recv,
    fx_send,
    fx_recv,
    s_send,
    s_recv,
    sb_send,
    sb_recv,
):
    count, rows, y_cells, z_cells = orb.shape
    block = core.shape[1]
    slow = bands // FAST
    stages = slow.bit_length() - 1
    chunk = x_in.shape[1] // x_recv.shape[0]
    chunks = rows // chunk
    firsts = fe_recv.shape[0] if chunks >= 8 else 0
    per_unit = TILE // chunk
    units = rows // (2 * TILE)
    groups = rows // bands
    per_group = bands // chunk
    pair_groups = 2 * TILE // bands
    me = lax.axis_index("band")
    slab = lax.axis_index("grid")
    spin = lax.axis_index("spin")
    place, fast = lax.div(me, FAST), lax.rem(me, FAST)
    bits = [lax.rem(lax.div(place, 2**k), 2) for k in range(stages)]
    start, ranges = 0, []
    for k in range(stages):
        size = slow >> (k + 1)
        ranges.append((size, start + bits[k] * size, start + (1 - bits[k]) * size))
        start = start + bits[k] * size
    spot = start
    across = {"band": place * FAST + (1 - fast)}
    twin = {"spin": 1 - spin}
    my_block = pl.ds(pl.multiple_of(me * block, TILE), block)

    def remote(src, dst, send, recv, device):
        return pltpu.make_async_remote_copy(
            src_ref=src,
            dst_ref=dst,
            send_sem=send,
            recv_sem=recv,
            device_id=device,
            device_id_type=MESH,
        )

    def take(ref, sem):
        pltpu.make_async_copy(ref, ref, sem).wait()

    def each(number, body):
        lax.fori_loop(0, number, lambda i, carry: (body(i), carry)[1], 0)

    def chunk_span(c):
        return pl.ds(c * chunk, chunk)

    def unit_rows(w):
        return pl.ds(pl.multiple_of(w * TILE, TILE), TILE)

    def line_rows(w):
        return pl.ds(pl.multiple_of(slab * rows + w * TILE, TILE), TILE)

    def band_block(j):
        return pl.ds(pl.multiple_of(j * block, TILE), block)

    def turned(value):
        return jnp.transpose(value, (1, 0, 2))

    def orb_copy(c):
        span = chunk_span(c)
        return pltpu.make_async_copy(orb_hbm.at[0, :, span], orb.at[:, span], orb_sem.at[c])

    def core_copy():
        return pltpu.make_async_copy(core_hbm.at[:, my_block], core, core_sem)

    def x_copy(c):
        span = chunk_span(c)
        return remote(part.at[1 - fast, :, span], x_in.at[:, span], x_send, x_recv.at[c], across)

    def stage_peer(k):
        return {"band": (place + (1 - 2 * bits[k]) * 2**k) * FAST + fast}

    def stage_room(k):
        size = ranges[k][0]
        return pl.ds(slow - 2 * size, size)

    def z_copy(c, k):
        span = chunk_span(c)
        size, keep, give = ranges[k]
        return remote(
            z_out.at[pl.ds(give, size), span],
            z_in.at[stage_room(k), span],
            z_send,
            z_recv.at[c, k],
            stage_peer(k),
        )

    def f_copy(n, k):
        size, keep, give = ranges[k]
        return remote(
            part.at[:, pl.ds(give, size), chunk_span(n)],
            f_in.at[n, :, stage_room(k)],
            f_send,
            f_recv.at[n, k],
            stage_peer(k),
        )

    def fe_copy(n):
        return remote(
            part.at[1 - fast, spot, chunk_span(n)],
            fx_in.at[n],
            fe_send.at[n],
            fe_recv.at[n],
            across,
        )

    def out_copy(i):
        span = pl.ds(i * bands, bands)
        return pltpu.make_async_copy(base.at[span], out_ref.at[span], out_sem.at[i])

    def table_copy(t):
        src, dst = [(tx_hbm, tx), (ty_hbm, ty), (tz_hbm, tz)][t]
        return pltpu.make_async_copy(src, dst, table_sem.at[t])

    def gather_copy(w, k):
        return remote(
            gx.at[0, :, line_rows(w)],
            gx.at[0, :, line_rows(w)],
            g_send.at[w, k - 1],
            g_recv.at[w, k - 1],
            {"grid": lax.rem(slab + k, grids)},
        )

    def n_copy(v):
        return remote(
            own.at[unit_rows(2 * v + 1 - spin)], n_twin.at[v], n_send.at[v], n_recv.at[v], twin
        )

    def nx_copy(v):
        return remote(
            nx.at[unit_rows(2 * v + 1 - spin)], nx_twin.at[v], nx_send.at[v], nx_recv.at[v], twin
        )

    def fx_same(v, k):
        return remote(
            gx.at[1, :, line_rows(2 * v + spin)],
            gx.at[1, :, line_rows(2 * v + spin)],
            fx_send.at[0, v, k],
            fx_recv.at[0, v, k],
            {"grid": lax.rem(slab + k, grids)},
        )

    def fx_cross(v, k):
        return remote(
            fx_out.at[v],
            gx.at[1, :, line_rows(2 * v + spin)],
            fx_send.at[1, v, k],
            fx_recv.at[1, v, k],
            {"spin": 1 - spin, "grid": lax.rem(slab + k, grids)},
        )

    def s_copy(v):
        return remote(
            s_out.at[v], base.at[unit_rows(2 * v + spin)], s_send.at[v], s_recv.at[v], twin
        )

    def my_row(i):
        row = i * bands + me
        unit = lax.div(row, TILE)
        return row, lax.rem(unit, 2), lax.div(unit, 2), lax.rem(row, TILE)

    def yb_copy(i, j, send):
        row, holder, v, e = my_row(i)
        slot = jnp.where(holder == spin, 0, 1)
        return remote(
            hy.at[0, i, band_block(j)],
            ny.at[slot, v, e],
            send,
            yb_recv.at[slot, v, e],
            {"spin": holder, "band": j},
        )

    def fy_own(v, e, i, q):
        return remote(
            fy.at[0, v, e],
            gy.at[1, i, my_block],
            fy_send.at[v, e],
            fy_recv.at[i, 0],
            {"band": q},
        )

    def fy_cross(v, e, i, q):
        return remote(
            fy.at[1, v, e],
            gy.at[1, i, my_block],
            fy_other,
            fy_recv.at[i, jnp.where(q == me, 1, 0)],
            {"spin": 1 - spin, "band": q},
        )

    def sb_copy(i, k):
        q = lax.rem(me + k, bands)
        return remote(
            hy.at[1, i, band_block(q)],
            sy.at[i * bands + me],
            sb_send,
            sb_recv.at[i],
            {"band": q},
        )

    each(chunks, lambda c: orb_copy(c).start())
    core_copy().start()
    for t in range(3):
        table_copy(t).start()
    barrier = pltpu.get_barrier_semaphore()
    beside = [(place > 0, place - 1), (place < slow - 1, place + 1)]
    partners = [twin, across] + [{"grid": lax.rem(slab + k, grids)} for k in range(1, grids)]
    for target in partners:
        pl.semaphore_signal(barrier, inc=1, device_id=target, device_id_type=MESH)
    for there, where in beside:

        @pl.when(there)
        def _():
            pl.semaphore_signal(
                barrier, inc=1, device_id={"band": where * FAST + fast}, device_id_type=MESH
            )

    neighbours = len(partners) + jnp.where(place > 0, 1, 0) + jnp.where(place < slow - 1, 1, 0)

    turns = slow - 1

    def call_on(turn):
        if turn == turns - 1:
            pl.semaphore_signal(across_sem, inc=1, device_id=across, device_id_type=MESH)
            return
        for side, (there, where) in enumerate(beside):

            @pl.when(there)
            def _():
                pl.semaphore_signal(
                    line_sem.at[turn, 1 - side],
                    inc=1,
                    device_id={"band": where * FAST + fast},
                    device_id_type=MESH,
                )

    def hear(turn):
        if turn == turns - 1:
            pl.semaphore_wait(across_sem, 1)
            return
        for side, (there, where) in enumerate(beside):

            @pl.when(there)
            def _():
                pl.semaphore_wait(line_sem.at[turn, side], 1)

        call_on(turn + 1)

    first = pairs_ref[0, 0]
    last = first + pairs_ref[0, 1]
    weights = []
    for n in range(count):
        ident = me * count + n
        weights.append(jnp.where((ident >= first) & (ident < last), 0.5, 1.0).astype(jnp.float32))

    reverse = [sum((d >> k & 1) << (stages - 1 - k) for k in range(stages)) for d in range(slow)]

    def squares(c):
        orb_copy(c).wait()
        for r in range(chunk):
            row = c * chunk + r
            for b in range(bands):
                total = jnp.zeros((block, z_cells), jnp.float32)
                for n in range(count):
                    values = orb[n, row, b * block : (b + 1) * block].astype(jnp.float32)
                    total += weights[n] * (values * values)
                part[b % FAST, reverse[b // FAST], row] = total

    def sum_across(c):
        x_copy(c).wait_recv()
        span = chunk_span(c)
        z_out[:, span] = part[fast, :, span] + x_in[:, span]
        z_copy(c, 0).start()

    def stage(k, c):
        span = chunk_span(c)
        z_copy(c, k).wait_recv()
        size, keep, give = ranges[k]
        z_out[pl.ds(keep, size), span] += z_in[stage_room(k), span]
        if k + 1 < stages:
            z_copy(c, k + 1).start()

    def first_stage(k, n):
        span = chunk_span(n)
        f_copy(n, k).wait_recv()
        size, keep, give = ranges[k]
        part[:, pl.ds(keep, size), span] += f_in[n, :, stage_room(k)]
        if k + 1 < stages:
            f_copy(n, k + 1).start()
        else:
            fe_copy(n).start()

    def first_end(n):
        fe_copy(n).wait_recv()
        collect(n, part[fast, spot, chunk_span(n)] + fx_in[n])
        if (n + 1) % per_unit == 0:
            share(n // per_unit)

    def collect(c, total):
        span = chunk_span(c)
        own[span] = 0.5 * core[span] + total
        for r in range(chunk):
            row = c * chunk + r
            i, q = lax.div(row, bands), lax.rem(row, bands)

            @pl.when(q != me)
            def _():
                remote(
                    own.at[row], gy.at[0, i, my_block], yf_send, yf_recv.at[i], {"band": q}
                ).start()

            @pl.when(q == me)
            def _():
                gy[0, i, my_block] = own[row]

    def share(w):
        v = lax.div(w, 2)
        gx[0, :, line_rows(w)] = turned(own[unit_rows(w)])
        for k in range(1, grids):
            gather_copy(w, k).start()

        @pl.when(lax.rem(w, 2) != spin)
        def _():
            n_copy(v).start()

        @pl.when(lax.rem(w, 2) == spin)
        def _():
            field = own[unit_rows(w)].reshape(TILE * block, z_cells)
            dz[0, v] = from_right(field, tz[...]).reshape(TILE, block, z_cells)

    def steep_second(i):
        take(gy.at[0, i, pl.ds(0, (bands - 1) * block)], yf_recv.at[i])
        hy[0, i] = from_left(ty[...], gy[0, i])
        for k in range(1, bands):
            yb_copy(i, lax.rem(me + k, bands), yb_send).start()
        row, holder, v, e = my_row(i)

        @pl.when(holder == spin)
        def _():
            ny[0, v, e] = hy[0, i, my_block]

        @pl.when(holder != spin)
        def _():
            yb_copy(i, me, yb_twin.at[i]).start()

    def along_first(t):
        table = tx[slab]
        for y in range(0, block, 2):
            pair = jnp.concatenate([gx[t, y], gx[t, y + 1]], axis=1)
            product = from_left(table, pair)
            hx[y] = product[:, :z_cells]
            hx[y + 1] = product[:, z_cells:]

    ahead = min(AHEAD, chunks)
    left = chunks - firsts
    order = [firsts] + [c for n in range(1, ahead) for c in (n - 1, firsts + n) if c != n - 1 or n <= firsts]
    order += list(range(ahead - 1, firsts))
    for at, c in enumerate(order):
        squares(c)
        if at == 0:
            pl.semaphore_wait(barrier, neighbours)
        if c < firsts:
            f_copy(c, 0).start()
        else:
            x_copy(c).start()
    call_on(0)
    end = left + stages
    inside = max(min((chunks - LATE) // per_group, groups - AFTER), 0)
    first_groups = firsts // per_group
    finish_first = FIRST_STEP * stages + ahead + FIRST_LAG

    def step(u):
        @pl.when(u + ahead < left)
        def _():
            squares(firsts + u + ahead)
            x_copy(firsts + u + ahead).start()

        @pl.when(u < left)
        def _():
            sum_across(firsts + u)

        for turn in range(turns):

            @pl.when(u == min(turn, stages))
            def _():
                hear(turn)

        for k in range(stages):

            @pl.when((u > k) & (u < left + k + 1))
            def _():
                stage(k, firsts + u - k - 1)

        @pl.when(u == stages)
        def _():
            core_copy().wait()
            for t in range(3):
                table_copy(t).wait()

        done = u - stages

        @pl.when((done >= 0) & (done < left))
        def _():
            c = firsts + done
            collect(c, z_out[spot, chunk_span(c)])

            @pl.when(lax.rem(c, per_unit) == per_unit - 1)
            def _():
                share(lax.div(c, per_unit))

        for n in range(firsts):
            for k in range(stages):

                @pl.when(u == 1 + FIRST_STEP * k + n)
                def _():
                    first_stage(k, n)

            @pl.when(u == finish_first + n)
            def _():
                first_end(n)

        for g in range(first_groups):

            @pl.when(u == finish_first + (g + 1) * per_group - 1 + FIRST_LATE)
            def _():
                steep_second(g)

        late = firsts + done - LATE

        @pl.when(
            (late >= firsts)
            & (late < inside * per_group)
            & (lax.rem(late, per_group) == per_group - 1)
        )
        def _():
            steep_second(lax.div(late, per_group))

    each(end, step)

    for v in range(units):
        n_copy(v).wait_recv()
        field = n_twin[v].reshape(TILE * block, z_cells)
        dz[1, v] = from_right(field, tz[...]).reshape(TILE, block, z_cells)
    for w in range(2 * units):
        for k in range(1, grids):
            gather_copy(w, k).wait_recv()
    along_first(0)
    nx[...] = turned(hx[...])
    for v in range(units):
        nx_copy(v).start()
    each(groups - inside, lambda g: steep_second(inside + g))

    def potential_rows(v, e):
        span = pl.ds(e, XC_ROWS)
        here = pl.ds((2 * v + spin) * TILE + e, XC_ROWS)
        n_own, n_other = own[here], n_twin[v, span]
        g_own = [nx[here], ny[0, v, span], dz[0, v, span]]
        g_other = [nx_twin[v, span], ny[1, v, span], dz[1, v, span]]
        s_own = g_own[0] * g_own[0] + g_own[1] * g_own[1] + g_own[2] * g_own[2]
        s_mix = g_own[0] * g_other[0] + g_own[1] * g_other[1] + g_own[2] * g_other[2]
        s_other = g_other[0] * g_other[0] + g_other[1] * g_other[1] + g_other[2] * g_other[2]
        energy, pull = jax.vjp(xc_energy, n_own, n_other, s_own, s_mix, s_other)
        derivs = pull(jnp.ones_like(energy))
        base[here] = derivs[0]
        s_out[v, span] = derivs[1]
        flux = [
            [2.0 * derivs[2] * g_own[a] + derivs[3] * g_other[a] for a in range(3)],
            [2.0 * derivs[4] * g_other[a] + derivs[3] * g_own[a] for a in range(3)],
        ]
        for slot in range(2):
            fx[slot, span] = flux[slot][0]
            fy[slot, v, span] = flux[slot][1]
            fz[slot, span] = flux[slot][2]
        for r in range(XC_ROWS):
            row = (2 * v + spin) * TILE + e + r
            i, q = lax.div(row, bands), lax.rem(row, bands)
            fy_cross(v, e + r, i, q).start()

            @pl.when(q != me)
            def _():
                fy_own(v, e + r, i, q).start()

            @pl.when(q == me)
            def _():
                gy[1, i, my_block] = fy[0, v, e + r]

    def evaluate(v):
        for e in range(TILE):
            row = (2 * v + spin) * TILE + e

            @pl.when(lax.rem(row, bands) != me)
            def _():
                take(ny.at[0, v, e], yb_recv.at[0, v, e])

            take(ny.at[1, v, e], yb_recv.at[1, v, e])
        nx_copy(v).wait_recv()
        each(TILE // XC_ROWS, lambda e: potential_rows(v, e * XC_ROWS))
        gx[1, :, line_rows(2 * v + spin)] = turned(fx[0])
        fx_out[v] = turned(fx[1])
        for k in range(grids):
            if k > 0:
                fx_same(v, k).start()
            fx_cross(v, k).start()
        for slot in range(2):
            field = fz[slot].reshape(TILE * block, z_cells)
            slope = from_right(field, tz[...]).reshape(TILE, block, z_cells)
            if slot == 0:
                mine = unit_rows(2 * v + spin)
                base[mine] = base[mine] - slope
            else:
                s_out[v] = s_out[v] - slope
        s_copy(v).start()

    def flux_second(i):
        take(gy.at[1, i, pl.ds(0, (bands - 1) * block)], fy_recv.at[i, 0])
        row, holder, v, e = my_row(i)

        @pl.when(holder != spin)
        def _():
            take(gy.at[1, i, pl.ds(0, block)], fy_recv.at[i, 1])

        hy[1, i] = from_left(ty[...], gy[1, i])
        for k in range(1, bands):
            sb_copy(i, k).start()
        sy[row] = hy[1, i, my_block]

    def unit_step(v):
        evaluate(v)

        @pl.when(v >= BEHIND)
        def _():
            each(pair_groups, lambda g: flux_second((v - BEHIND) * pair_groups + g))

    each(units, unit_step)
    behind = min(BEHIND, units) * pair_groups
    each(behind, lambda g: flux_second(groups - behind + g))

    for v in range(units):
        for k in range(grids):
            if k > 0:
                fx_same(v, k).wait_recv()
            fx_cross(v, k).wait_recv()
    along_first(1)
    for v in range(units):
        s_copy(v).wait_recv()
    base[...] = base[...] - turned(hx[...])

    take(part.at[0, :, pl.ds(0, left * chunk)], x_send)
    take(z_out.at[pl.ds(0, slow - 1), pl.ds(0, left * chunk)], z_send)
    if firsts:
        take(part.at[:, pl.ds(0, slow - 1), pl.ds(0, firsts * chunk)], f_send)
    for n in range(firsts):
        fe_copy(n).wait_send()
    take(own.at[pl.ds(0, rows - groups)], yf_send)
    take(sy.at[pl.ds(0, groups * (bands - 1))], yb_send)
    for g in range(groups):
        row, holder, v, e = my_row(g)

        @pl.when(holder != spin)
        def _():
            take(sy.at[0], yb_twin.at[g])

    take(fy.at[1], fy_other)

    def drain(v):
        n_copy(v).wait_send()
        nx_copy(v).wait_send()
        s_copy(v).wait_send()
        for k in range(grids):
            if k > 0:
                fx_same(v, k).wait_send()
                gather_copy(2 * v, k).wait_send()
                gather_copy(2 * v + 1, k).wait_send()
            fx_cross(v, k).wait_send()
        for e in range(TILE):
            row = (2 * v + spin) * TILE + e

            @pl.when(lax.rem(row, bands) != me)
            def _():
                take(fy.at[0, v, e], fy_send.at[v, e])

    each(units, drain)

    def finish(i):
        take(sy.at[pl.ds(0, bands - 1)], sb_recv.at[i])
        span = pl.ds(i * bands, bands)
        base[span] = base[span] - sy[span]
        out_copy(i).start()

    each(groups, finish)
    each(groups, lambda i: out_copy(i).wait())
    take(sy.at[pl.ds(0, groups * (bands - 1))], sb_send)


def potential_call(orbitals, partial_bands, core_density, tables):
    bands, grids = lax.axis_size("band"), lax.axis_size("grid")
    _, count, rows, y_cells, z_cells = orbitals.shape
    block, slow = y_cells // bands, bands // FAST
    stages = slow.bit_length() - 1
    x_cells = rows * grids
    chunk = min(CHUNK, TILE)
    chunks = rows // chunk
    units, groups = rows // (2 * TILE), rows // bands
    hbm = pl.BlockSpec(memory_space=pl.ANY)
    dma = pltpu.SemaphoreType.DMA
    real = jnp.float32

    def held(*shape):
        return pltpu.VMEM(shape + (z_cells,), real)

    return pl.pallas_call(
        functools.partial(potential_kernel, bands, grids),
        out_shape=jax.ShapeDtypeStruct((rows, block, z_cells), real),
        in_specs=[pl.BlockSpec(memory_space=pltpu.SMEM)] + [hbm] * 5,
        out_specs=hbm,
        scratch_shapes=[
            pltpu.VMEM((count, rows, y_cells, z_cells), jnp.bfloat16),
            held(rows, block),
            held(FAST, slow, rows, block),
            held(slow, rows, block),
            held(slow, rows, block),
            held(slow - 1, rows, block),
            held(FIRSTS, FAST, slow - 1, chunk, block),
            held(FIRSTS, chunk, block),
            *[pltpu.VMEM(table.shape, table.dtype) for table in tables],
            held(rows, block),
            held(2, block, x_cells),
            held(block, rows),
            held(rows, block),
            held(2, groups, y_cells),
            held(2, groups, y_cells),
            held(2, units, TILE, block),
            held(2, units, TILE, block),
            held(units, TILE, block),
            held(units, TILE, block),
            held(2, TILE, block),
            held(units, block, TILE),
            held(2, units, TILE, block),
            held(2, TILE, block),
            held(units, TILE, block),
            held(rows, block),
            held(rows, block),
            dma((chunks,)),
            dma,
            dma,
            dma((chunks,)),
            dma,
            dma((chunks, stages)),
            dma,
            dma((FIRSTS, stages)),
            dma((FIRSTS,)),
            dma((FIRSTS,)),
            dma((3,)),
            dma((groups,)),
            pltpu.SemaphoreType.REGULAR((max(slow - 2, 1), 2)),
            pltpu.SemaphoreType.REGULAR,
            dma((2 * units, grids - 1)),
            dma((2 * units, grids - 1)),
            dma((units,)),
            dma((units,)),
            dma((units,)),
            dma((units,)),
            dma,
            dma((groups,)),
            dma,
            dma((groups,)),
            dma((2, units, TILE)),
            dma((units, TILE)),
            dma,
            dma((groups, 2)),
            dma((2, units, grids)),
            dma((2, units, grids)),
            dma((units,)),
            dma((units,)),
            dma,
            dma((groups,)),
        ],
        compiler_params=pltpu.CompilerParams(
            collective_id=0, has_side_effects=True, vmem_limit_bytes=60 * 2**20
        ),
        name="potential",
    )(partial_bands, orbitals, core_density, *tables)


def per_device(orbitals, partial_bands, core_density):
    rows, y_cells, z_cells = core_density.shape
    grids = lax.axis_size("grid")
    table = spectral_table(rows * grids)
    slabs = [left_table(table[g * rows : (g + 1) * rows]) for g in range(grids)]
    tables = (
        jnp.asarray(np.stack(slabs)),
        jnp.asarray(left_table(spectral_table(y_cells))),
        jnp.asarray(right_table(spectral_table(z_cells).T)),
    )
    return potential_call(orbitals, partial_bands, core_density, tables)[None]


def solution(mesh):
    in_specs = (P("spin", "band", "grid", None, None), P("spin", None), P("grid", None, None))
    out_specs = P("spin", "grid", "band", None)
    return jax.shard_map(
        per_device, mesh=mesh, in_specs=in_specs, out_specs=out_specs, check_vma=False
    )
```

```python
import functools
import math

import jax
import jax.numpy as jnp
import numpy as np
from jax import lax
from jax.experimental import pallas as pl
from jax.experimental.pallas import tpu as pltpu
from jax.sharding import PartitionSpec as P

KAPPA = 0.804
MU_X = 0.2195149727645171
BETA = 0.06672455060314922
GAMMA = (1.0 - math.log(2.0)) / math.pi**2
FZ_NORM = 2.0 ** (4.0 / 3.0) - 2.0
FPP_ZERO = 1.709921
MESH = pl.DeviceIdType.MESH
CHUNK = 4
AHEAD = 3
LATE = 2
AFTER = 1
BEHIND = 3
FIRSTS = 2
FIRST_STEP = 2
FIRST_LAG = 3
DEPTH = 6
FIRST_LATE = 3
FAST = 2
XC_ROWS = 2
TILE = 8


def cube_root(value):
    return jnp.exp(jnp.log(value) * (1.0 / 3.0))


def pw_fit(radius, root, amp, alpha, beta_one, beta_two, beta_three, beta_four):
    denom = (2.0 * amp) * (
        root * (beta_one + root * (beta_two + root * (beta_three + root * beta_four)))
    )
    return -2.0 * amp * (1.0 + alpha * radius) * jnp.log(1.0 + 1.0 / denom)


def exchange_part(double, sigma_four):
    kfermi = (3.0 * math.pi**2) ** (1.0 / 3.0) * cube_root(double)
    product = kfermi * double
    scaled = sigma_four / (4.0 * product * product)
    enhance = 1.0 + KAPPA - KAPPA / (1.0 + MU_X * scaled / KAPPA)
    return -0.75 / math.pi * product * enhance


def xc_energy(n_up, n_down, s_uu, s_ud, s_dd):
    exch = 0.5 * (exchange_part(2.0 * n_up, 4.0 * s_uu) + exchange_part(2.0 * n_down, 4.0 * s_dd))
    total = n_up + n_down
    zeta = (n_up - n_down) / total
    third = cube_root(total)
    radius = (3.0 / (4.0 * math.pi)) ** (1.0 / 3.0) / third
    root = jnp.sqrt(radius)
    ec_para = pw_fit(radius, root, 0.031091, 0.2137, 7.5957, 3.5876, 1.6382, 0.49294)
    ec_ferro = pw_fit(radius, root, 0.015545, 0.20548, 14.1189, 6.1977, 3.3662, 0.62517)
    neg_stiff = pw_fit(radius, root, 0.016887, 0.11125, 10.357, 3.6231, 0.88026, 0.49671)
    plus_z = 1.0 + zeta
    minus_z = 1.0 - zeta
    plus_third = cube_root(plus_z)
    minus_third = cube_root(minus_z)
    fzeta = (plus_z * plus_third + minus_z * minus_third - 2.0) * (1.0 / FZ_NORM)
    zeta_sq = zeta * zeta
    zeta_four = zeta_sq * zeta_sq
    ec_lda = (
        ec_para
        - neg_stiff * fzeta * (1.0 / FPP_ZERO) * (1.0 - zeta_four)
        + (ec_ferro - ec_para) * fzeta * zeta_four
    )
    phi = 0.5 * (plus_third * plus_third + minus_third * minus_third)
    phi_cube = phi * phi * phi
    kfermi = (3.0 * math.pi**2) ** (1.0 / 3.0) * third
    screen_sq = kfermi * (4.0 / math.pi)
    sigma = s_uu + 2.0 * s_ud + s_dd
    tsq = sigma / (4.0 * phi * phi * screen_sq * total * total)
    amp = BETA / GAMMA / (jnp.exp(-ec_lda / (GAMMA * phi_cube)) - 1.0)
    atsq = amp * tsq
    gradient_term = (
        GAMMA
        * phi_cube
        * jnp.log(1.0 + BETA / GAMMA * tsq * (1.0 + atsq) / (1.0 + atsq + atsq * atsq))
    )
    return exch + total * (ec_lda + gradient_term)


def spectral_table(length):
    index = np.arange(length)
    angle = 2.0 * np.pi / length * (index[:, None] * index[None, :] % length)
    mode = np.where(index < length // 2, index, index - length)
    mode = np.where(index == length // 2, 0, mode)
    wave = 2.0 * np.pi / length * mode
    sines, cosines = np.sin(angle), np.cos(angle)
    first_term = (sines * wave[None, :]) @ cosines.T
    second_term = (cosines * wave[None, :]) @ sines.T
    return (second_term - first_term) / length


def halves_of_table(table):
    high = table.astype(jnp.bfloat16)
    low = (table - high.astype(np.float64)).astype(jnp.bfloat16)
    return high, low


def left_table(table):
    high, low = halves_of_table(table)
    return np.concatenate([np.concatenate([part, part], axis=1) for part in (high, low)], axis=0)


def right_table(table):
    high, low = halves_of_table(table)
    both = np.concatenate([high, low], axis=1)
    return np.concatenate([both, both], axis=0)


def halves(field):
    high = field.astype(jnp.bfloat16)
    return high, (field - high.astype(jnp.float32)).astype(jnp.bfloat16)


def from_left(table, field):
    product = jnp.dot(
        table, jnp.concatenate(halves(field), axis=0), preferred_element_type=jnp.float32
    )
    rows = product.shape[0] // 2
    return product[:rows] + product[rows:]


def from_right(field, table):
    product = jnp.dot(
        jnp.concatenate(halves(field), axis=1), table, preferred_element_type=jnp.float32
    )
    columns = product.shape[1] // 2
    return product[:, :columns] + product[:, columns:]


def potential_kernel(
    bands,
    grids,
    pairs_ref,
    orb_hbm,
    core_hbm,
    tx_hbm,
    ty_hbm,
    tz_hbm,
    out_ref,
    orb,
    core,
    part,
    x_in,
    z_out,
    z_in,
    f_in,
    fx_in,
    tx,
    ty,
    tz,
    own,
    gx,
    hx,
    nx,
    gy,
    hy,
    ny,
    dz,
    n_twin,
    nx_twin,
    fx,
    fx_out,
    fy,
    fz,
    s_out,
    base,
    sy,
    orb_sem,
    core_sem,
    x_send,
    x_recv,
    z_send,
    z_recv,
    f_send,
    f_recv,
    fe_send,
    fe_recv,
    table_sem,
    out_sem,
    line_sem,
    across_sem,
    g_send,
    g_recv,
    n_send,
    n_recv,
    nx_send,
    nx_recv,
    yf_send,
    yf_recv,
    yb_send,
    yb_twin,
    yb_recv,
    fy_send,
    fy_other,
    fy_recv,
    fx_send,
    fx_recv,
    s_send,
    s_recv,
    sb_send,
    sb_recv,
):
    count, rows, y_cells, z_cells = orb.shape
    block = core.shape[1]
    slow = bands // FAST
    stages = slow.bit_length() - 1
    chunk = x_in.shape[1] // x_recv.shape[0]
    chunks = rows // chunk
    firsts = fe_recv.shape[0] if chunks >= 8 else 0
    per_unit = TILE // chunk
    depth = orb_sem.shape[0]
    units = rows // (2 * TILE)
    groups = rows // bands
    per_group = bands // chunk
    pair_groups = 2 * TILE // bands
    me = lax.axis_index("band")
    slab = lax.axis_index("grid")
    spin = lax.axis_index("spin")
    place, fast = lax.div(me, FAST), lax.rem(me, FAST)
    bits = [lax.rem(lax.div(place, 2**k), 2) for k in range(stages)]
    start, ranges = 0, []
    for k in range(stages):
        size = slow >> (k + 1)
        ranges.append((size, start + bits[k] * size, start + (1 - bits[k]) * size))
        start = start + bits[k] * size
    spot = start
    across = {"band": place * FAST + (1 - fast)}
    twin = {"spin": 1 - spin}
    my_block = pl.ds(pl.multiple_of(me * block, TILE), block)

    def remote(src, dst, send, recv, device):
        return pltpu.make_async_remote_copy(
            src_ref=src,
            dst_ref=dst,
            send_sem=send,
            recv_sem=recv,
            device_id=device,
            device_id_type=MESH,
        )

    def take(ref, sem):
        pltpu.make_async_copy(ref, ref, sem).wait()

    mine = True if bands == TILE else lax.rem(lax.div(me, TILE), 2) == spin

    def take_rows(ref, ones, sem):
        full = ref.shape[0]
        if bands == TILE:
            take(ref.at[pl.ds(0, full - ones)], sem)
        else:

            @pl.when(mine)
            def _():
                take(ref.at[pl.ds(0, full - ones)], sem)

            @pl.when(jnp.logical_not(mine))
            def _():
                take(ref, sem)

    def each(number, body):
        lax.fori_loop(0, number, lambda i, carry: (body(i), carry)[1], 0)

    def chunk_span(c):
        return pl.ds(c * chunk, chunk)

    def unit_rows(w):
        return pl.ds(pl.multiple_of(w * TILE, TILE), TILE)

    def line_rows(w):
        return pl.ds(pl.multiple_of(slab * rows + w * TILE, TILE), TILE)

    def band_block(j):
        return pl.ds(pl.multiple_of(j * block, TILE), block)

    def turned(value):
        return jnp.transpose(value, (1, 0, 2))

    def orb_copy(c):
        span = chunk_span(c)
        return pltpu.make_async_copy(orb_hbm.at[0, :, span], orb.at[:, span], orb_sem.at[lax.rem(c, depth)])

    def core_copy():
        return pltpu.make_async_copy(core_hbm.at[:, my_block], core, core_sem)

    def x_copy(c):
        span = chunk_span(c)
        return remote(part.at[1 - fast, :, span], x_in.at[:, span], x_send, x_recv.at[c], across)

    def stage_peer(k):
        return {"band": (place + (1 - 2 * bits[k]) * 2**k) * FAST + fast}

    def stage_room(k):
        size = ranges[k][0]
        return pl.ds(slow - 2 * size, size)

    def z_copy(c, k):
        span = chunk_span(c)
        size, keep, give = ranges[k]
        return remote(
            z_out.at[pl.ds(give, size), span],
            z_in.at[stage_room(k), span],
            z_send,
            z_recv.at[c, k],
            stage_peer(k),
        )

    def f_copy(n, k):
        size, keep, give = ranges[k]
        return remote(
            part.at[:, pl.ds(give, size), chunk_span(n)],
            f_in.at[n, :, stage_room(k)],
            f_send,
            f_recv.at[n, k],
            stage_peer(k),
        )

    def fe_copy(n):
        return remote(
            part.at[1 - fast, spot, chunk_span(n)],
            fx_in.at[n],
            fe_send.at[n],
            fe_recv.at[n],
            across,
        )

    def out_copy(i):
        span = pl.ds(i * bands, bands)
        return pltpu.make_async_copy(base.at[span], out_ref.at[span], out_sem)

    def table_copy(t):
        src, dst = [(tx_hbm, tx), (ty_hbm, ty), (tz_hbm, tz)][t]
        return pltpu.make_async_copy(src, dst, table_sem.at[t])

    def gather_copy(w, k):
        return remote(
            gx.at[0, :, line_rows(w)],
            gx.at[0, :, line_rows(w)],
            g_send,
            g_recv,
            {"grid": lax.rem(slab + k, grids)},
        )

    def n_copy(v):
        return remote(
            own.at[unit_rows(2 * v + 1 - spin)], n_twin.at[v], n_send, n_recv, twin
        )

    def nx_copy(v):
        return remote(
            nx.at[unit_rows(2 * v + 1 - spin)], nx_twin.at[v], nx_send, nx_recv.at[v], twin
        )

    def fx_same(v, k):
        return remote(
            gx.at[1, :, line_rows(2 * v + spin)],
            gx.at[1, :, line_rows(2 * v + spin)],
            fx_send.at[0],
            fx_recv,
            {"grid": lax.rem(slab + k, grids)},
        )

    def fx_cross(v, k):
        return remote(
            fx_out.at[v],
            gx.at[1, :, line_rows(2 * v + spin)],
            fx_send.at[1],
            fx_recv,
            {"spin": 1 - spin, "grid": lax.rem(slab + k, grids)},
        )

    def s_copy(v):
        return remote(
            s_out.at[v], base.at[unit_rows(2 * v + spin)], s_send, s_recv, twin
        )

    def my_row(i):
        row = i * bands + me
        unit = lax.div(row, TILE)
        return row, lax.rem(unit, 2), lax.div(unit, 2), lax.rem(row, TILE)

    def yb_copy(i, j, send):
        row, holder, v, e = my_row(i)
        slot = jnp.where(holder == spin, 0, 1)
        return remote(
            hy.at[0, i, band_block(j)],
            ny.at[slot, v, e],
            send,
            yb_recv.at[slot, v],
            {"spin": holder, "band": j},
        )

    def fy_own(v, e, i, q):
        return remote(
            fy.at[0, v, e],
            gy.at[1, i, my_block],
            fy_send,
            fy_recv.at[i, 0],
            {"band": q},
        )

    def fy_cross(v, e, i, q):
        return remote(
            fy.at[1, v, e],
            gy.at[1, i, my_block],
            fy_other,
            fy_recv.at[i, jnp.where(q == me, 1, 0)],
            {"spin": 1 - spin, "band": q},
        )

    def sb_copy(i, k):
        q = lax.rem(me + k, bands)
        return remote(
            hy.at[1, i, band_block(q)],
            sy.at[i * bands + me],
            sb_send,
            sb_recv.at[i],
            {"band": q},
        )

    each(depth, lambda c: orb_copy(c).start())
    core_copy().start()
    for t in range(3):
        table_copy(t).start()
    barrier = pltpu.get_barrier_semaphore()
    beside = [(place > 0, place - 1), (place < slow - 1, place + 1)]
    partners = [twin, across] + [{"grid": lax.rem(slab + k, grids)} for k in range(1, grids)]
    for target in partners:
        pl.semaphore_signal(barrier, inc=1, device_id=target, device_id_type=MESH)
    for there, where in beside:

        @pl.when(there)
        def _():
            pl.semaphore_signal(
                barrier, inc=1, device_id={"band": where * FAST + fast}, device_id_type=MESH
            )

    neighbours = len(partners) + jnp.where(place > 0, 1, 0) + jnp.where(place < slow - 1, 1, 0)

    turns = slow - 1

    def call_on(turn):
        if turn == turns - 1:
            pl.semaphore_signal(across_sem, inc=1, device_id=across, device_id_type=MESH)
            return
        for side, (there, where) in enumerate(beside):

            @pl.when(there)
            def _():
                pl.semaphore_signal(
                    line_sem.at[turn, 1 - side],
                    inc=1,
                    device_id={"band": where * FAST + fast},
                    device_id_type=MESH,
                )

    def hear(turn):
        if turn == turns - 1:
            pl.semaphore_wait(across_sem, 1)
            return
        for side, (there, where) in enumerate(beside):

            @pl.when(there)
            def _():
                pl.semaphore_wait(line_sem.at[turn, side], 1)

        call_on(turn + 1)

    first = pairs_ref[0, 0]
    last = first + pairs_ref[0, 1]
    weights = []
    for n in range(count):
        ident = me * count + n
        weights.append(jnp.where((ident >= first) & (ident < last), 0.5, 1.0).astype(jnp.float32))

    reverse = [sum((d >> k & 1) << (stages - 1 - k) for k in range(stages)) for d in range(slow)]

    def squares(c):
        orb_copy(c).wait()
        for r in range(chunk):
            row = c * chunk + r
            for b in range(bands):
                total = jnp.zeros((block, z_cells), jnp.float32)
                for n in range(count):
                    values = orb[n, row, b * block : (b + 1) * block].astype(jnp.float32)
                    total += weights[n] * (values * values)
                part[b % FAST, reverse[b // FAST], row] = total

        @pl.when(c + depth < chunks)
        def _():
            orb_copy(c + depth).start()

    def sum_across(c):
        x_copy(c).wait_recv()
        span = chunk_span(c)
        z_out[:, span] = part[fast, :, span] + x_in[:, span]
        z_copy(c, 0).start()

    def stage(k, c):
        span = chunk_span(c)
        z_copy(c, k).wait_recv()
        size, keep, give = ranges[k]
        z_out[pl.ds(keep, size), span] += z_in[stage_room(k), span]
        if k + 1 < stages:
            z_copy(c, k + 1).start()

    def first_stage(k, n):
        span = chunk_span(n)
        f_copy(n, k).wait_recv()
        size, keep, give = ranges[k]
        part[:, pl.ds(keep, size), span] += f_in[n, :, stage_room(k)]
        if k + 1 < stages:
            f_copy(n, k + 1).start()
        else:
            fe_copy(n).start()

    def first_end(n):
        fe_copy(n).wait_recv()
        collect(n, part[fast, spot, chunk_span(n)] + fx_in[n])
        if (n + 1) % per_unit == 0:
            share(n // per_unit)

    def collect(c, total):
        span = chunk_span(c)
        own[span] = 0.5 * core[span] + total
        for r in range(chunk):
            row = c * chunk + r
            i, q = lax.div(row, bands), lax.rem(row, bands)

            @pl.when(q != me)
            def _():
                remote(
                    own.at[row], gy.at[0, i, my_block], yf_send, yf_recv.at[i], {"band": q}
                ).start()

            @pl.when(q == me)
            def _():
                gy[0, i, my_block] = own[row]

    def share(w):
        v = lax.div(w, 2)
        gx[0, :, line_rows(w)] = turned(own[unit_rows(w)])
        for k in range(1, grids):
            gather_copy(w, k).start()

        @pl.when(lax.rem(w, 2) != spin)
        def _():
            n_copy(v).start()

        @pl.when(lax.rem(w, 2) == spin)
        def _():
            field = own[unit_rows(w)].reshape(TILE * block, z_cells)
            dz[0, v] = from_right(field, tz[...]).reshape(TILE, block, z_cells)

    def steep_second(i):
        take(gy.at[0, i, pl.ds(0, (bands - 1) * block)], yf_recv.at[i])
        hy[0, i] = from_left(ty[...], gy[0, i])
        for k in range(1, bands):
            yb_copy(i, lax.rem(me + k, bands), yb_send).start()
        row, holder, v, e = my_row(i)

        @pl.when(holder == spin)
        def _():
            ny[0, v, e] = hy[0, i, my_block]

        @pl.when(holder != spin)
        def _():
            yb_copy(i, me, yb_twin).start()

    def along_first(t):
        table = tx[slab]
        for y in range(0, block, 2):
            pair = jnp.concatenate([gx[t, y], gx[t, y + 1]], axis=1)
            product = from_left(table, pair)
            hx[y] = product[:, :z_cells]
            hx[y + 1] = product[:, z_cells:]

    ahead = min(AHEAD, chunks)
    left = chunks - firsts
    order = [firsts] + [c for n in range(1, ahead) for c in (n - 1, firsts + n) if c != n - 1 or n <= firsts]
    order += list(range(ahead - 1, firsts))
    for at, c in enumerate(order):
        squares(c)
        if at == 0:
            pl.semaphore_wait(barrier, neighbours)
        if c < firsts:
            f_copy(c, 0).start()
        else:
            x_copy(c).start()
    call_on(0)
    end = left + stages
    inside = max(min((chunks - LATE) // per_group, groups - AFTER), 0)
    first_groups = firsts // per_group
    finish_first = FIRST_STEP * stages + ahead + FIRST_LAG

    def step(u):
        @pl.when(u + ahead < left)
        def _():
            squares(firsts + u + ahead)
            x_copy(firsts + u + ahead).start()

        @pl.when(u < left)
        def _():
            sum_across(firsts + u)

        for turn in range(turns):

            @pl.when(u == min(turn, stages))
            def _():
                hear(turn)

        for k in range(stages):

            @pl.when((u > k) & (u < left + k + 1))
            def _():
                stage(k, firsts + u - k - 1)

        @pl.when(u == stages)
        def _():
            core_copy().wait()
            for t in range(3):
                table_copy(t).wait()

        done = u - stages

        @pl.when((done >= 0) & (done < left))
        def _():
            c = firsts + done
            collect(c, z_out[spot, chunk_span(c)])

            @pl.when(lax.rem(c, per_unit) == per_unit - 1)
            def _():
                share(lax.div(c, per_unit))

        for n in range(firsts):
            for k in range(stages):

                @pl.when(u == 1 + FIRST_STEP * k + n)
                def _():
                    first_stage(k, n)

            @pl.when(u == finish_first + n)
            def _():
                first_end(n)

        for g in range(first_groups):

            @pl.when(u == finish_first + (g + 1) * per_group - 1 + FIRST_LATE)
            def _():
                steep_second(g)

        late = firsts + done - LATE

        @pl.when(
            (late >= firsts)
            & (late < inside * per_group)
            & (lax.rem(late, per_group) == per_group - 1)
        )
        def _():
            steep_second(lax.div(late, per_group))

    each(end, step)

    take(n_twin, n_recv)
    for v in range(units):
        field = n_twin[v].reshape(TILE * block, z_cells)
        dz[1, v] = from_right(field, tz[...]).reshape(TILE, block, z_cells)
    take(gx.at[0, :, pl.ds(0, (grids - 1) * rows)], g_recv)
    along_first(0)
    nx[...] = turned(hx[...])
    for v in range(units):
        nx_copy(v).start()
    each(groups - inside, lambda g: steep_second(inside + g))

    def potential_rows(v, e):
        span = pl.ds(e, XC_ROWS)
        here = pl.ds((2 * v + spin) * TILE + e, XC_ROWS)
        n_own, n_other = own[here], n_twin[v, span]
        g_own = [nx[here], ny[0, v, span], dz[0, v, span]]
        g_other = [nx_twin[v, span], ny[1, v, span], dz[1, v, span]]
        s_own = g_own[0] * g_own[0] + g_own[1] * g_own[1] + g_own[2] * g_own[2]
        s_mix = g_own[0] * g_other[0] + g_own[1] * g_other[1] + g_own[2] * g_other[2]
        s_other = g_other[0] * g_other[0] + g_other[1] * g_other[1] + g_other[2] * g_other[2]
        energy, pull = jax.vjp(xc_energy, n_own, n_other, s_own, s_mix, s_other)
        derivs = pull(jnp.ones_like(energy))
        base[here] = derivs[0]
        s_out[v, span] = derivs[1]
        flux = [
            [2.0 * derivs[2] * g_own[a] + derivs[3] * g_other[a] for a in range(3)],
            [2.0 * derivs[4] * g_other[a] + derivs[3] * g_own[a] for a in range(3)],
        ]
        for slot in range(2):
            fx[slot, span] = flux[slot][0]
            fy[slot, v, span] = flux[slot][1]
            fz[slot, span] = flux[slot][2]
        for r in range(XC_ROWS):
            row = (2 * v + spin) * TILE + e + r
            i, q = lax.div(row, bands), lax.rem(row, bands)
            fy_cross(v, e + r, i, q).start()

            @pl.when(q != me)
            def _():
                fy_own(v, e + r, i, q).start()

            @pl.when(q == me)
            def _():
                gy[1, i, my_block] = fy[0, v, e + r]

    def evaluate(v):
        take_rows(ny.at[0, v], 1, yb_recv.at[0, v])
        take(ny.at[1, v], yb_recv.at[1, v])
        nx_copy(v).wait_recv()
        each(TILE // XC_ROWS, lambda e: potential_rows(v, e * XC_ROWS))
        gx[1, :, line_rows(2 * v + spin)] = turned(fx[0])
        fx_out[v] = turned(fx[1])
        for k in range(grids):
            if k > 0:
                fx_same(v, k).start()
            fx_cross(v, k).start()
        for slot in range(2):
            field = fz[slot].reshape(TILE * block, z_cells)
            slope = from_right(field, tz[...]).reshape(TILE, block, z_cells)
            if slot == 0:
                mine = unit_rows(2 * v + spin)
                base[mine] = base[mine] - slope
            else:
                s_out[v] = s_out[v] - slope
        s_copy(v).start()

    def flux_second(i):
        take(gy.at[1, i, pl.ds(0, (bands - 1) * block)], fy_recv.at[i, 0])
        row, holder, v, e = my_row(i)

        @pl.when(holder != spin)
        def _():
            take(gy.at[1, i, pl.ds(0, block)], fy_recv.at[i, 1])

        hy[1, i] = from_left(ty[...], gy[1, i])
        for k in range(1, bands):
            sb_copy(i, k).start()
        sy[row] = hy[1, i, my_block]

    def unit_step(v):
        evaluate(v)

        @pl.when(v >= BEHIND)
        def _():
            each(pair_groups, lambda g: flux_second((v - BEHIND) * pair_groups + g))

    each(units, unit_step)
    behind = min(BEHIND, units) * pair_groups
    each(behind, lambda g: flux_second(groups - behind + g))

    take(gx.at[1, :, pl.ds(0, (2 * grids - 1) * units * TILE)], fx_recv)
    along_first(1)
    take(s_out, s_recv)
    base[...] = base[...] - turned(hx[...])

    take(part.at[0, :, pl.ds(0, left * chunk)], x_send)
    take(z_out.at[pl.ds(0, slow - 1), pl.ds(0, left * chunk)], z_send)
    if firsts:
        take(part.at[:, pl.ds(0, slow - 1), pl.ds(0, firsts * chunk)], f_send)
    for n in range(firsts):
        fe_copy(n).wait_send()
    take(own.at[pl.ds(0, rows - groups)], yf_send)
    take(sy.at[pl.ds(0, groups * (bands - 1))], yb_send)
    if bands == TILE:
        take(sy.at[pl.ds(0, units)], yb_twin)
    else:

        @pl.when(jnp.logical_not(mine))
        def _():
            take(sy.at[pl.ds(0, groups)], yb_twin)

    take(fy.at[1], fy_other)
    take_rows(sy.at[pl.ds(0, units * TILE)], units, fy_send)
    take(own.at[pl.ds(0, units * TILE)], n_send)
    take(own.at[pl.ds(0, units * TILE)], nx_send)
    take(s_out, s_send)
    take(gx.at[0, :, pl.ds(0, (grids - 1) * rows)], g_send)
    take(gx.at[1, :, pl.ds(0, (grids - 1) * units * TILE)], fx_send.at[0])
    take(gx.at[1, :, pl.ds(0, grids * units * TILE)], fx_send.at[1])

    def finish(i):
        take(sy.at[pl.ds(0, bands - 1)], sb_recv.at[i])
        span = pl.ds(i * bands, bands)
        base[span] = base[span] - sy[span]
        out_copy(i).start()

    each(groups, finish)
    take(base, out_sem)
    take(sy.at[pl.ds(0, groups * (bands - 1))], sb_send)


def potential_call(orbitals, partial_bands, core_density, tables):
    bands, grids = lax.axis_size("band"), lax.axis_size("grid")
    _, count, rows, y_cells, z_cells = orbitals.shape
    block, slow = y_cells // bands, bands // FAST
    stages = slow.bit_length() - 1
    x_cells = rows * grids
    chunk = min(CHUNK, TILE)
    chunks = rows // chunk
    units, groups = rows // (2 * TILE), rows // bands
    hbm = pl.BlockSpec(memory_space=pl.ANY)
    dma = pltpu.SemaphoreType.DMA
    real = jnp.float32

    def held(*shape):
        return pltpu.VMEM(shape + (z_cells,), real)

    return pl.pallas_call(
        functools.partial(potential_kernel, bands, grids),
        out_shape=jax.ShapeDtypeStruct((rows, block, z_cells), real),
        in_specs=[pl.BlockSpec(memory_space=pltpu.SMEM)] + [hbm] * 5,
        out_specs=hbm,
        scratch_shapes=[
            pltpu.VMEM((count, rows, y_cells, z_cells), jnp.bfloat16),
            held(rows, block),
            held(FAST, slow, rows, block),
            held(slow, rows, block),
            held(slow, rows, block),
            held(slow - 1, rows, block),
            held(FIRSTS, FAST, slow - 1, chunk, block),
            held(FIRSTS, chunk, block),
            *[pltpu.VMEM(table.shape, table.dtype) for table in tables],
            held(rows, block),
            held(2, block, x_cells),
            held(block, rows),
            held(rows, block),
            held(2, groups, y_cells),
            held(2, groups, y_cells),
            held(2, units, TILE, block),
            held(2, units, TILE, block),
            held(units, TILE, block),
            held(units, TILE, block),
            held(2, TILE, block),
            held(units, block, TILE),
            held(2, units, TILE, block),
            held(2, TILE, block),
            held(units, TILE, block),
            held(rows, block),
            held(rows, block),
            dma((min(DEPTH, chunks),)),
            dma,
            dma,
            dma((chunks,)),
            dma,
            dma((chunks, stages)),
            dma,
            dma((FIRSTS, stages)),
            dma((FIRSTS,)),
            dma((FIRSTS,)),
            dma((3,)),
            dma,
            pltpu.SemaphoreType.REGULAR((max(slow - 2, 1), 2)),
            pltpu.SemaphoreType.REGULAR,
            dma,
            dma,
            dma,
            dma,
            dma,
            dma((units,)),
            dma,
            dma((groups,)),
            dma,
            dma,
            dma((2, units)),
            dma,
            dma,
            dma((groups, 2)),
            dma((2,)),
            dma,
            dma,
            dma,
            dma,
            dma((groups,)),
        ],
        compiler_params=pltpu.CompilerParams(
            collective_id=0, has_side_effects=True, vmem_limit_bytes=60 * 2**20
        ),
        name="potential",
    )(partial_bands, orbitals, core_density, *tables)


def per_device(orbitals, partial_bands, core_density):
    rows, y_cells, z_cells = core_density.shape
    grids = lax.axis_size("grid")
    table = spectral_table(rows * grids)
    slabs = [left_table(table[g * rows : (g + 1) * rows]) for g in range(grids)]
    tables = (
        jnp.asarray(np.stack(slabs)),
        jnp.asarray(left_table(spectral_table(y_cells))),
        jnp.asarray(right_table(spectral_table(z_cells).T)),
    )
    return potential_call(orbitals, partial_bands, core_density, tables)[None]


def solution(mesh):
    in_specs = (P("spin", "band", "grid", None, None), P("spin", None), P("grid", None, None))
    out_specs = P("spin", "grid", "band", None)
    return jax.shard_map(
        per_device, mesh=mesh, in_specs=in_specs, out_specs=out_specs, check_vma=False
    )
```

```python
import functools
import math

import jax
import jax.numpy as jnp
import numpy as np
from jax import lax
from jax.experimental import pallas as pl
from jax.experimental.pallas import tpu as pltpu
from jax.sharding import PartitionSpec as P

KAPPA = 0.804
MU_X = 0.2195149727645171
BETA = 0.06672455060314922
GAMMA = (1.0 - math.log(2.0)) / math.pi**2
FZ_NORM = 2.0 ** (4.0 / 3.0) - 2.0
FPP_ZERO = 1.709921
MESH = pl.DeviceIdType.MESH
CHUNK = 4
AHEAD = 4
LATE = 3
AFTER = 1
BEHIND = 3
FIRSTS = 2
FIRST_STEP = 2
FIRST_LAG = 2
DEPTH = 6
FIRST_LATE = 3
FAST = 2
XC_ROWS = 2
TILE = 8


def cube_root(value):
    return jnp.exp(jnp.log(value) * (1.0 / 3.0))


def pw_fit(radius, root, amp, alpha, beta_one, beta_two, beta_three, beta_four):
    denom = (2.0 * amp) * (
        root * (beta_one + root * (beta_two + root * (beta_three + root * beta_four)))
    )
    return -2.0 * amp * (1.0 + alpha * radius) * jnp.log(1.0 + 1.0 / denom)


def exchange_part(double, sigma_four):
    kfermi = (3.0 * math.pi**2) ** (1.0 / 3.0) * cube_root(double)
    product = kfermi * double
    scaled = sigma_four / (4.0 * product * product)
    enhance = 1.0 + KAPPA - KAPPA / (1.0 + MU_X * scaled / KAPPA)
    return -0.75 / math.pi * product * enhance


def xc_energy(n_up, n_down, s_uu, s_ud, s_dd):
    exch = 0.5 * (exchange_part(2.0 * n_up, 4.0 * s_uu) + exchange_part(2.0 * n_down, 4.0 * s_dd))
    total = n_up + n_down
    zeta = (n_up - n_down) / total
    third = cube_root(total)
    radius = (3.0 / (4.0 * math.pi)) ** (1.0 / 3.0) / third
    root = jnp.sqrt(radius)
    ec_para = pw_fit(radius, root, 0.031091, 0.2137, 7.5957, 3.5876, 1.6382, 0.49294)
    ec_ferro = pw_fit(radius, root, 0.015545, 0.20548, 14.1189, 6.1977, 3.3662, 0.62517)
    neg_stiff = pw_fit(radius, root, 0.016887, 0.11125, 10.357, 3.6231, 0.88026, 0.49671)
    plus_z = 1.0 + zeta
    minus_z = 1.0 - zeta
    plus_third = cube_root(plus_z)
    minus_third = cube_root(minus_z)
    fzeta = (plus_z * plus_third + minus_z * minus_third - 2.0) * (1.0 / FZ_NORM)
    zeta_sq = zeta * zeta
    zeta_four = zeta_sq * zeta_sq
    ec_lda = (
        ec_para
        - neg_stiff * fzeta * (1.0 / FPP_ZERO) * (1.0 - zeta_four)
        + (ec_ferro - ec_para) * fzeta * zeta_four
    )
    phi = 0.5 * (plus_third * plus_third + minus_third * minus_third)
    phi_cube = phi * phi * phi
    kfermi = (3.0 * math.pi**2) ** (1.0 / 3.0) * third
    screen_sq = kfermi * (4.0 / math.pi)
    sigma = s_uu + 2.0 * s_ud + s_dd
    tsq = sigma / (4.0 * phi * phi * screen_sq * total * total)
    amp = BETA / GAMMA / (jnp.exp(-ec_lda / (GAMMA * phi_cube)) - 1.0)
    atsq = amp * tsq
    gradient_term = (
        GAMMA
        * phi_cube
        * jnp.log(1.0 + BETA / GAMMA * tsq * (1.0 + atsq) / (1.0 + atsq + atsq * atsq))
    )
    return exch + total * (ec_lda + gradient_term)


def spectral_table(length):
    index = np.arange(length)
    angle = 2.0 * np.pi / length * (index[:, None] * index[None, :] % length)
    mode = np.where(index < length // 2, index, index - length)
    mode = np.where(index == length // 2, 0, mode)
    wave = 2.0 * np.pi / length * mode
    sines, cosines = np.sin(angle), np.cos(angle)
    first_term = (sines * wave[None, :]) @ cosines.T
    second_term = (cosines * wave[None, :]) @ sines.T
    return (second_term - first_term) / length


def halves_of_table(table):
    high = table.astype(jnp.bfloat16)
    low = (table - high.astype(np.float64)).astype(jnp.bfloat16)
    return high, low


def left_table(table):
    high, low = halves_of_table(table)
    return np.concatenate([np.concatenate([part, part], axis=1) for part in (high, low)], axis=0)


def right_table(table):
    high, low = halves_of_table(table)
    both = np.concatenate([high, low], axis=1)
    return np.concatenate([both, both], axis=0)


def halves(field):
    high = field.astype(jnp.bfloat16)
    return high, (field - high.astype(jnp.float32)).astype(jnp.bfloat16)


def from_left(table, field):
    product = jnp.dot(
        table, jnp.concatenate(halves(field), axis=0), preferred_element_type=jnp.float32
    )
    rows = product.shape[0] // 2
    return product[:rows] + product[rows:]


def from_right(field, table):
    product = jnp.dot(
        jnp.concatenate(halves(field), axis=1), table, preferred_element_type=jnp.float32
    )
    columns = product.shape[1] // 2
    return product[:, :columns] + product[:, columns:]


def potential_kernel(
    bands,
    grids,
    pairs_ref,
    orb_hbm,
    core_hbm,
    tx_hbm,
    ty_hbm,
    tz_hbm,
    out_ref,
    orb,
    core,
    part,
    x_in,
    z_out,
    z_in,
    f_in,
    fx_in,
    tx,
    ty,
    tz,
    own,
    gx,
    hx,
    nx,
    gy,
    hy,
    ny,
    dz,
    n_twin,
    nx_twin,
    fx,
    fx_out,
    fy,
    fz,
    s_out,
    base,
    sy,
    orb_sem,
    core_sem,
    x_send,
    x_recv,
    z_send,
    z_recv,
    f_send,
    f_recv,
    fe_send,
    fe_recv,
    table_sem,
    out_sem,
    line_sem,
    across_sem,
    g_send,
    g_recv,
    n_send,
    n_recv,
    nx_send,
    nx_recv,
    yf_send,
    yf_recv,
    yb_send,
    yb_twin,
    yb_recv,
    fy_send,
    fy_other,
    fy_recv,
    fx_send,
    fx_recv,
    s_send,
    s_recv,
    sb_send,
    sb_recv,
):
    count, rows, y_cells, z_cells = orb.shape
    block = core.shape[1]
    slow = bands // FAST
    stages = slow.bit_length() - 1
    chunk = min(CHUNK, TILE)
    chunks = rows // chunk
    firsts = fe_recv.shape[0] if chunks >= 8 else 0
    per_unit = TILE // chunk
    depth = orb_sem.shape[0]
    units = rows // (2 * TILE)
    groups = rows // bands
    per_group = bands // chunk
    pair_groups = 2 * TILE // bands
    me = lax.axis_index("band")
    slab = lax.axis_index("grid")
    spin = lax.axis_index("spin")
    place, fast = lax.div(me, FAST), lax.rem(me, FAST)
    bits = [lax.rem(lax.div(place, 2**k), 2) for k in range(stages)]
    start, ranges = 0, []
    for k in range(stages):
        size = slow >> (k + 1)
        ranges.append((size, start + bits[k] * size, start + (1 - bits[k]) * size))
        start = start + bits[k] * size
    spot = start
    across = {"band": place * FAST + (1 - fast)}
    twin = {"spin": 1 - spin}
    my_block = pl.ds(pl.multiple_of(me * block, TILE), block)

    def remote(src, dst, send, recv, device):
        return pltpu.make_async_remote_copy(
            src_ref=src,
            dst_ref=dst,
            send_sem=send,
            recv_sem=recv,
            device_id=device,
            device_id_type=MESH,
        )

    def take(ref, sem):
        pltpu.make_async_copy(ref, ref, sem).wait()

    mine = True if bands == TILE else lax.rem(lax.div(me, TILE), 2) == spin

    def take_rows(ref, ones, sem):
        full = ref.shape[0]
        if bands == TILE:
            take(ref.at[pl.ds(0, full - ones)], sem)
        else:

            @pl.when(mine)
            def _():
                take(ref.at[pl.ds(0, full - ones)], sem)

            @pl.when(jnp.logical_not(mine))
            def _():
                take(ref, sem)

    def each(number, body):
        lax.fori_loop(0, number, lambda i, carry: (body(i), carry)[1], 0)

    def chunk_span(c):
        return pl.ds(c * chunk, chunk)

    def unit_rows(w):
        return pl.ds(pl.multiple_of(w * TILE, TILE), TILE)

    def line_rows(w):
        return pl.ds(pl.multiple_of(slab * rows + w * TILE, TILE), TILE)

    def band_block(j):
        return pl.ds(pl.multiple_of(j * block, TILE), block)

    def turned(value):
        return jnp.transpose(value, (1, 0, 2))

    def orb_copy(c):
        span = chunk_span(c)
        return pltpu.make_async_copy(orb_hbm.at[0, :, span], orb.at[:, span], orb_sem.at[lax.rem(c, depth)])

    def core_copy():
        return pltpu.make_async_copy(core_hbm.at[:, my_block], core, core_sem)

    def x_copy(c):
        span = chunk_span(c)
        return remote(part.at[1 - fast, :, span], x_in.at[:, span], x_send, x_recv.at[lax.rem(c, x_recv.shape[0])], across)

    def stage_peer(k):
        return {"band": (place + (1 - 2 * bits[k]) * 2**k) * FAST + fast}

    def stage_room(k):
        size = ranges[k][0]
        return pl.ds(slow - 2 * size, size)

    def z_copy(c, k):
        span = chunk_span(c)
        size, keep, give = ranges[k]
        return remote(
            z_out.at[pl.ds(give, size), span],
            z_in.at[stage_room(k), span],
            z_send,
            z_recv.at[lax.rem(c, z_recv.shape[0]), k],
            stage_peer(k),
        )

    def f_copy(n, k):
        size, keep, give = ranges[k]
        return remote(
            part.at[:, pl.ds(give, size), chunk_span(n)],
            f_in.at[n, :, stage_room(k)],
            f_send,
            f_recv.at[n, k],
            stage_peer(k),
        )

    def fe_copy(n):
        return remote(
            part.at[1 - fast, spot, chunk_span(n)],
            fx_in.at[n],
            fe_send.at[n],
            fe_recv.at[n],
            across,
        )

    def out_copy(i):
        span = pl.ds(i * bands, bands)
        return pltpu.make_async_copy(base.at[span], out_ref.at[span], out_sem)

    def table_copy(t):
        src, dst = [(tx_hbm, tx), (ty_hbm, ty), (tz_hbm, tz)][t]
        return pltpu.make_async_copy(src, dst, table_sem.at[t])

    def gather_copy(w, k):
        return remote(
            gx.at[0, :, line_rows(w)],
            gx.at[0, :, line_rows(w)],
            g_send,
            g_recv,
            {"grid": lax.rem(slab + k, grids)},
        )

    def n_copy(v):
        return remote(
            own.at[unit_rows(2 * v + 1 - spin)], n_twin.at[v], n_send, n_recv, twin
        )

    def nx_copy(v):
        return remote(
            nx.at[unit_rows(2 * v + 1 - spin)], nx_twin.at[v], nx_send, nx_recv.at[v], twin
        )

    def fx_same(v, k):
        return remote(
            gx.at[1, :, line_rows(2 * v + spin)],
            gx.at[1, :, line_rows(2 * v + spin)],
            fx_send.at[0],
            fx_recv,
            {"grid": lax.rem(slab + k, grids)},
        )

    def fx_cross(v, k):
        return remote(
            fx_out.at[v],
            gx.at[1, :, line_rows(2 * v + spin)],
            fx_send.at[1],
            fx_recv,
            {"spin": 1 - spin, "grid": lax.rem(slab + k, grids)},
        )

    def s_copy(v):
        return remote(
            s_out.at[v], base.at[unit_rows(2 * v + spin)], s_send, s_recv, twin
        )

    def my_row(i):
        row = i * bands + me
        unit = lax.div(row, TILE)
        return row, lax.rem(unit, 2), lax.div(unit, 2), lax.rem(row, TILE)

    def yb_copy(i, j, send):
        row, holder, v, e = my_row(i)
        slot = jnp.where(holder == spin, 0, 1)
        return remote(
            hy.at[0, i, band_block(j)],
            ny.at[slot, v, e],
            send,
            yb_recv.at[slot, v],
            {"spin": holder, "band": j},
        )

    def fy_own(v, e, i, q):
        return remote(
            fy.at[0, v, e],
            gy.at[1, i, my_block],
            fy_send,
            fy_recv.at[i],
            {"band": q},
        )

    def fy_cross(v, e, i, q):
        return remote(
            fy.at[1, v, e],
            gy.at[1, i, my_block],
            fy_other,
            fy_recv.at[i],
            {"spin": 1 - spin, "band": q},
        )

    def sb_copy(i, k):
        q = lax.rem(me + k, bands)
        return remote(
            hy.at[1, i, band_block(q)],
            sy.at[i * bands + me],
            sb_send,
            sb_recv.at[i],
            {"band": q},
        )

    each(depth, lambda c: orb_copy(c).start())
    core_copy().start()
    for t in range(3):
        table_copy(t).start()
    barrier = pltpu.get_barrier_semaphore()
    beside = [(place > 0, place - 1), (place < slow - 1, place + 1)]
    partners = [twin, across] + [{"grid": lax.rem(slab + k, grids)} for k in range(1, grids)]
    for target in partners:
        pl.semaphore_signal(barrier, inc=1, device_id=target, device_id_type=MESH)
    for there, where in beside:

        @pl.when(there)
        def _():
            pl.semaphore_signal(
                barrier, inc=1, device_id={"band": where * FAST + fast}, device_id_type=MESH
            )

    neighbours = len(partners) + jnp.where(place > 0, 1, 0) + jnp.where(place < slow - 1, 1, 0)

    turns = slow - 1

    def call_on(turn):
        if turn == turns - 1:
            pl.semaphore_signal(across_sem, inc=1, device_id=across, device_id_type=MESH)
            return
        for side, (there, where) in enumerate(beside):

            @pl.when(there)
            def _():
                pl.semaphore_signal(
                    line_sem.at[turn, 1 - side],
                    inc=1,
                    device_id={"band": where * FAST + fast},
                    device_id_type=MESH,
                )

    def hear(turn):
        if turn == turns - 1:
            pl.semaphore_wait(across_sem, 1)
            return
        for side, (there, where) in enumerate(beside):

            @pl.when(there)
            def _():
                pl.semaphore_wait(line_sem.at[turn, side], 1)

        call_on(turn + 1)

    first = pairs_ref[0, 0]
    last = first + pairs_ref[0, 1]
    weights = []
    for n in range(count):
        ident = me * count + n
        weights.append(jnp.where((ident >= first) & (ident < last), 0.5, 1.0).astype(jnp.float32))

    reverse = [sum((d >> k & 1) << (stages - 1 - k) for k in range(stages)) for d in range(slow)]

    def squares(c):
        orb_copy(c).wait()
        for r in range(chunk):
            row = c * chunk + r
            for b in range(bands):
                total = jnp.zeros((block, z_cells), jnp.float32)
                for n in range(count):
                    values = orb[n, row, b * block : (b + 1) * block].astype(jnp.float32)
                    total += weights[n] * (values * values)
                part[b % FAST, reverse[b // FAST], row] = total

        @pl.when(c + depth < chunks)
        def _():
            orb_copy(c + depth).start()

    def sum_across(c):
        x_copy(c).wait_recv()
        span = chunk_span(c)
        z_out[:, span] = part[fast, :, span] + x_in[:, span]
        z_copy(c, 0).start()

    def stage(k, c):
        span = chunk_span(c)
        z_copy(c, k).wait_recv()
        size, keep, give = ranges[k]
        z_out[pl.ds(keep, size), span] += z_in[stage_room(k), span]
        if k + 1 < stages:
            z_copy(c, k + 1).start()

    def first_stage(k, n):
        span = chunk_span(n)
        f_copy(n, k).wait_recv()
        size, keep, give = ranges[k]
        part[:, pl.ds(keep, size), span] += f_in[n, :, stage_room(k)]
        if k + 1 < stages:
            f_copy(n, k + 1).start()
        else:
            fe_copy(n).start()

    def first_end(n):
        fe_copy(n).wait_recv()
        collect(n, part[fast, spot, chunk_span(n)] + fx_in[n])
        if (n + 1) % per_unit == 0:
            share(n // per_unit)

    def collect(c, total):
        span = chunk_span(c)
        own[span] = 0.5 * core[span] + total
        for r in range(chunk):
            row = c * chunk + r
            i, q = lax.div(row, bands), lax.rem(row, bands)

            @pl.when(q != me)
            def _():
                remote(
                    own.at[row], gy.at[0, i, my_block], yf_send, yf_recv.at[i], {"band": q}
                ).start()

            @pl.when(q == me)
            def _():
                gy[0, i, my_block] = own[row]

    def share(w):
        v = lax.div(w, 2)
        gx[0, :, line_rows(w)] = turned(own[unit_rows(w)])
        for k in range(1, grids):
            gather_copy(w, k).start()

        @pl.when(lax.rem(w, 2) != spin)
        def _():
            n_copy(v).start()

        @pl.when(lax.rem(w, 2) == spin)
        def _():
            field = own[unit_rows(w)].reshape(TILE * block, z_cells)
            dz[0, v] = from_right(field, tz[...]).reshape(TILE, block, z_cells)

    def steep_second(i):
        take(gy.at[0, i, pl.ds(0, (bands - 1) * block)], yf_recv.at[i])
        hy[0, i] = from_left(ty[...], gy[0, i])
        for k in range(1, bands):
            yb_copy(i, lax.rem(me + k, bands), yb_send).start()
        row, holder, v, e = my_row(i)

        @pl.when(holder == spin)
        def _():
            ny[0, v, e] = hy[0, i, my_block]

        @pl.when(holder != spin)
        def _():
            yb_copy(i, me, yb_twin).start()

    def along_first(t):
        table = tx[slab]
        for y in range(0, block, 2):
            pair = jnp.concatenate([gx[t, y], gx[t, y + 1]], axis=1)
            product = from_left(table, pair)
            hx[y] = product[:, :z_cells]
            hx[y + 1] = product[:, z_cells:]

    ahead = min(AHEAD, chunks)
    left = chunks - firsts
    order = [firsts] + [c for n in range(1, ahead) for c in (n - 1, firsts + n) if c != n - 1 or n <= firsts]
    order += list(range(ahead - 1, firsts))
    for at, c in enumerate(order):
        squares(c)
        if at == 0:
            pl.semaphore_wait(barrier, neighbours)
        if c < firsts:
            f_copy(c, 0).start()
        else:
            x_copy(c).start()
    call_on(0)
    end = left + stages
    inside = max(min((chunks - LATE) // per_group, groups - AFTER), 0)
    first_groups = firsts // per_group
    finish_first = FIRST_STEP * stages + ahead + FIRST_LAG

    def step(u):
        @pl.when(u + ahead < left)
        def _():
            squares(firsts + u + ahead)
            x_copy(firsts + u + ahead).start()

        @pl.when(u < left)
        def _():
            sum_across(firsts + u)

        for turn in range(turns):

            @pl.when(u == min(turn, stages))
            def _():
                hear(turn)

        for k in range(stages):

            @pl.when((u > k) & (u < left + k + 1))
            def _():
                stage(k, firsts + u - k - 1)

        @pl.when(u == stages)
        def _():
            core_copy().wait()
            for t in range(3):
                table_copy(t).wait()

        done = u - stages

        @pl.when((done >= 0) & (done < left))
        def _():
            c = firsts + done
            collect(c, z_out[spot, chunk_span(c)])

            @pl.when(lax.rem(c, per_unit) == per_unit - 1)
            def _():
                share(lax.div(c, per_unit))

        for n in range(firsts):
            for k in range(stages):

                @pl.when(u == 1 + FIRST_STEP * k + n)
                def _():
                    first_stage(k, n)

            @pl.when(u == finish_first + n)
            def _():
                first_end(n)

        for g in range(first_groups):

            @pl.when(u == finish_first + (g + 1) * per_group - 1 + FIRST_LATE)
            def _():
                steep_second(g)

        late = firsts + done - LATE

        @pl.when(
            (late >= firsts)
            & (late < inside * per_group)
            & (lax.rem(late, per_group) == per_group - 1)
        )
        def _():
            steep_second(lax.div(late, per_group))

    each(end, step)

    take(n_twin, n_recv)
    for v in range(units):
        field = n_twin[v].reshape(TILE * block, z_cells)
        dz[1, v] = from_right(field, tz[...]).reshape(TILE, block, z_cells)
    take(gx.at[0, :, pl.ds(0, (grids - 1) * rows)], g_recv)
    along_first(0)
    nx[...] = turned(hx[...])
    for v in range(units):
        nx_copy(v).start()
    each(groups - inside, lambda g: steep_second(inside + g))

    def potential_rows(v, e):
        span = pl.ds(e, XC_ROWS)
        here = pl.ds((2 * v + spin) * TILE + e, XC_ROWS)
        n_own, n_other = own[here], n_twin[v, span]
        g_own = [nx[here], ny[0, v, span], dz[0, v, span]]
        g_other = [nx_twin[v, span], ny[1, v, span], dz[1, v, span]]
        s_own = g_own[0] * g_own[0] + g_own[1] * g_own[1] + g_own[2] * g_own[2]
        s_mix = g_own[0] * g_other[0] + g_own[1] * g_other[1] + g_own[2] * g_other[2]
        s_other = g_other[0] * g_other[0] + g_other[1] * g_other[1] + g_other[2] * g_other[2]
        energy, pull = jax.vjp(xc_energy, n_own, n_other, s_own, s_mix, s_other)
        derivs = pull(jnp.ones_like(energy))
        base[here] = derivs[0]
        s_out[v, span] = derivs[1]
        flux = [
            [2.0 * derivs[2] * g_own[a] + derivs[3] * g_other[a] for a in range(3)],
            [2.0 * derivs[4] * g_other[a] + derivs[3] * g_own[a] for a in range(3)],
        ]
        for slot in range(2):
            fx[slot, span] = flux[slot][0]
            fy[slot, v, span] = flux[slot][1]
            fz[slot, span] = flux[slot][2]
        for r in range(XC_ROWS):
            row = (2 * v + spin) * TILE + e + r
            i, q = lax.div(row, bands), lax.rem(row, bands)
            fy_cross(v, e + r, i, q).start()

            @pl.when(q != me)
            def _():
                fy_own(v, e + r, i, q).start()

            @pl.when(q == me)
            def _():
                gy[1, i, my_block] = fy[0, v, e + r]

    def evaluate(v):
        take_rows(ny.at[0, v], 1, yb_recv.at[0, v])
        take(ny.at[1, v], yb_recv.at[1, v])
        nx_copy(v).wait_recv()
        each(TILE // XC_ROWS, lambda e: potential_rows(v, e * XC_ROWS))
        gx[1, :, line_rows(2 * v + spin)] = turned(fx[0])
        fx_out[v] = turned(fx[1])
        for k in range(grids):
            if k > 0:
                fx_same(v, k).start()
            fx_cross(v, k).start()
        for slot in range(2):
            field = fz[slot].reshape(TILE * block, z_cells)
            slope = from_right(field, tz[...]).reshape(TILE, block, z_cells)
            if slot == 0:
                mine = unit_rows(2 * v + spin)
                base[mine] = base[mine] - slope
            else:
                s_out[v] = s_out[v] - slope
        s_copy(v).start()

    def flux_second(i):
        row, holder, v, e = my_row(i)

        @pl.when(holder == spin)
        def _():
            take(gy.at[1, i, pl.ds(0, (bands - 1) * block)], fy_recv.at[i])

        @pl.when(holder != spin)
        def _():
            take(gy.at[1, i], fy_recv.at[i])

        hy[1, i] = from_left(ty[...], gy[1, i])
        for k in range(1, bands):
            sb_copy(i, k).start()
        sy[row] = hy[1, i, my_block]

    def unit_step(v):
        evaluate(v)

        @pl.when(v >= BEHIND)
        def _():
            each(pair_groups, lambda g: flux_second((v - BEHIND) * pair_groups + g))

    each(units, unit_step)
    behind = min(BEHIND, units) * pair_groups
    each(behind, lambda g: flux_second(groups - behind + g))

    take(gx.at[1, :, pl.ds(0, (2 * grids - 1) * units * TILE)], fx_recv)
    along_first(1)
    take(s_out, s_recv)
    base[...] = base[...] - turned(hx[...])

    take(part.at[0, :, pl.ds(0, left * chunk)], x_send)
    take(z_out.at[pl.ds(0, slow - 1), pl.ds(0, left * chunk)], z_send)
    if firsts:
        take(part.at[:, pl.ds(0, slow - 1), pl.ds(0, firsts * chunk)], f_send)
    for n in range(firsts):
        fe_copy(n).wait_send()
    take(own.at[pl.ds(0, rows - groups)], yf_send)
    take(sy.at[pl.ds(0, groups * (bands - 1))], yb_send)
    if bands == TILE:
        take(sy.at[pl.ds(0, units)], yb_twin)
    else:

        @pl.when(jnp.logical_not(mine))
        def _():
            take(sy.at[pl.ds(0, groups)], yb_twin)

    take(fy.at[1], fy_other)
    take_rows(sy.at[pl.ds(0, units * TILE)], units, fy_send)
    take(own.at[pl.ds(0, units * TILE)], n_send)
    take(own.at[pl.ds(0, units * TILE)], nx_send)
    take(s_out, s_send)
    take(gx.at[0, :, pl.ds(0, (grids - 1) * rows)], g_send)
    take(gx.at[1, :, pl.ds(0, (grids - 1) * units * TILE)], fx_send.at[0])
    take(gx.at[1, :, pl.ds(0, grids * units * TILE)], fx_send.at[1])

    def finish(i):
        take(sy.at[pl.ds(0, bands - 1)], sb_recv.at[i])
        span = pl.ds(i * bands, bands)
        base[span] = base[span] - sy[span]
        out_copy(i).start()

    each(groups, finish)
    take(base, out_sem)
    take(sy.at[pl.ds(0, groups * (bands - 1))], sb_send)


def potential_call(orbitals, partial_bands, core_density, tables):
    bands, grids = lax.axis_size("band"), lax.axis_size("grid")
    _, count, rows, y_cells, z_cells = orbitals.shape
    block, slow = y_cells // bands, bands // FAST
    stages = slow.bit_length() - 1
    x_cells = rows * grids
    chunk = min(CHUNK, TILE)
    chunks = rows // chunk
    units, groups = rows // (2 * TILE), rows // bands
    hbm = pl.BlockSpec(memory_space=pl.ANY)
    dma = pltpu.SemaphoreType.DMA
    real = jnp.float32

    def held(*shape):
        return pltpu.VMEM(shape + (z_cells,), real)

    return pl.pallas_call(
        functools.partial(potential_kernel, bands, grids),
        out_shape=jax.ShapeDtypeStruct((rows, block, z_cells), real),
        in_specs=[pl.BlockSpec(memory_space=pltpu.SMEM)] + [hbm] * 5,
        out_specs=hbm,
        scratch_shapes=[
            pltpu.VMEM((count, rows, y_cells, z_cells), jnp.bfloat16),
            held(rows, block),
            held(FAST, slow, rows, block),
            held(slow, rows, block),
            held(slow, rows, block),
            held(slow - 1, rows, block),
            held(FIRSTS, FAST, slow - 1, chunk, block),
            held(FIRSTS, chunk, block),
            *[pltpu.VMEM(table.shape, table.dtype) for table in tables],
            held(rows, block),
            held(2, block, x_cells),
            held(block, rows),
            held(rows, block),
            held(2, groups, y_cells),
            held(2, groups, y_cells),
            held(2, units, TILE, block),
            held(2, units, TILE, block),
            held(units, TILE, block),
            held(units, TILE, block),
            held(2, TILE, block),
            held(units, block, TILE),
            held(2, units, TILE, block),
            held(2, TILE, block),
            held(units, TILE, block),
            held(rows, block),
            held(rows, block),
            dma((min(DEPTH, chunks),)),
            dma,
            dma,
            dma((min(2 * AHEAD + 2, chunks),)),
            dma,
            dma((min(4, chunks), stages)),
            dma,
            dma((FIRSTS, stages)),
            dma((FIRSTS,)),
            dma((FIRSTS,)),
            dma((3,)),
            dma,
            pltpu.SemaphoreType.REGULAR((max(slow - 2, 1), 2)),
            pltpu.SemaphoreType.REGULAR,
            dma,
            dma,
            dma,
            dma,
            dma,
            dma((units,)),
            dma,
            dma((groups,)),
            dma,
            dma,
            dma((2, units)),
            dma,
            dma,
            dma((groups,)),
            dma((2,)),
            dma,
            dma,
            dma,
            dma,
            dma((groups,)),
        ],
        compiler_params=pltpu.CompilerParams(
            collective_id=0, has_side_effects=True, vmem_limit_bytes=60 * 2**20
        ),
        name="potential",
    )(partial_bands, orbitals, core_density, *tables)


def per_device(orbitals, partial_bands, core_density):
    rows, y_cells, z_cells = core_density.shape
    grids = lax.axis_size("grid")
    table = spectral_table(rows * grids)
    slabs = [left_table(table[g * rows : (g + 1) * rows]) for g in range(grids)]
    tables = (
        jnp.asarray(np.stack(slabs)),
        jnp.asarray(left_table(spectral_table(y_cells))),
        jnp.asarray(right_table(spectral_table(z_cells).T)),
    )
    return potential_call(orbitals, partial_bands, core_density, tables)[None]


def solution(mesh):
    in_specs = (P("spin", "band", "grid", None, None), P("spin", None), P("grid", None, None))
    out_specs = P("spin", "grid", "band", None)
    return jax.shard_map(
        per_device, mesh=mesh, in_specs=in_specs, out_specs=out_specs, check_vma=False
    )
```
